128 devices in a mesh: row: 8 (over x, core), col: 16 (over z, y).
Axes of the slice: x: 4, y: 4, z: 4, core: 2. Of those that a mesh axis runs over, the one named last changes fastest.
Arguments:
- spectrum: float32 [2, 33554432], P(None, ('row', 'col')), may hold values from -6 to 6
Outputs:
- product: float32 [2, 33554432], P(None, ('row', 'col'))
The draws below stay inside these ranges and needn't reach their ends.
All inputs are finite; a program needn't handle non-finite values.
Results may differ from the reference program's by a relative error of at most 0.000098.
Values sent between devices are 32-bit elements; how exact they have to be, the bound alone decides.
A program may use at most 64 MiB of HBM per device.

```python
import math
import jax
import jax.numpy as jnp

MODES = 33554432
POINTS = 50331648


def shard_levels(key, dims, shards, low, top_value):
    factor_of = 1.0
    for position, parts in shards:
        heights = jax.random.uniform(jax.random.fold_in(jax.random.fold_in(key, 6), position), (parts,), jnp.float32, low / len(shards), top_value / len(shards))
        factor_of = factor_of * jnp.repeat(jnp.exp(heights), dims[position] // parts).reshape((-1,) + (1,) * (len(dims) - 1 - position))
    return factor_of


def noise(own_key, extent, width, most, shards=(), held_as=jnp.bfloat16):
    drawn = jax.random.normal(own_key, extent, jnp.float32) * width
    if len(shards) > 0:
        drawn = shard_levels(own_key, extent, shards, -0.22, 0.18) * drawn
    return jnp.clip(drawn, min=-most, max=most).astype(held_as)


def setup_inputs(seed: int = 0) -> dict:
    splits = jax.random.split(jax.random.key(seed), 2)
    spectrum = noise(splits[0], (2, MODES), 1.0, 6.0, ((1, 128),), jnp.float32)
    return {"spectrum": spectrum}


def reference(spectrum):
    coeff = spectrum[0] + 1j * spectrum[1]
    half = MODES // 2
    gap = jnp.zeros((POINTS - MODES,), dtype=coeff.dtype)
    padded = jnp.concatenate([coeff[:half], gap, coeff[half:]])
    field = jnp.fft.ifft(padded) * (POINTS / math.sqrt(MODES))
    square = field * field
    transform = jnp.fft.fft(square) * (1.0 / math.sqrt(POINTS))
    kept = jnp.concatenate([transform[:half], transform[POINTS - half:]])
    return jnp.stack([jnp.real(kept), jnp.imag(kept)]).astype(jnp.float32)
```

```python
import functools
import math

import jax
import jax.numpy as jnp
import numpy as np
from jax import lax
from jax.experimental import pallas as pl
from jax.experimental.pallas import tpu as pltpu
from jax.sharding import PartitionSpec as P

B = 131072
MODES = 33554432
POINTS = 50331648
DEVICES = 128
STEP = 37

MESH = pl.DeviceIdType.MESH
F32 = jnp.float32
BF16 = jnp.bfloat16


def unit(turns, total):
    angle = 2.0 * np.pi * (np.asarray(turns, np.int64) % total) / total
    return np.cos(angle), np.sin(angle)


def tables():
    m = np.arange(128)
    lane = np.arange(128)
    cos, sin = unit(m[:, None] * m[None, :], 128)
    plus = np.block([[cos, -sin], [sin, cos]])
    both = np.stack([plus, plus.T]).astype(np.float32)
    high = both.astype(BF16)
    low = (both - high.astype(np.float32)).astype(BF16)
    lanes = np.zeros((3, 2, 128, 128), np.float32)
    place = np.zeros((3, 2, 128, 128), np.float32)
    columns = np.zeros((4, 128, 128), np.float32)
    for i in range(3):
        mine = i + 3 * m
        lanes[i] = unit(mine[:, None] * lane[None, :], POINTS)
        place[i] = unit(mine[:, None] * lane[None, :] * 1024, POINTS)
        re, im = unit(mine[:, None] * np.arange(8)[None, :] * 128, POINTS)
        columns[i, :, 0:8], columns[i, :, 8:16] = re, im
        columns[i, :, 16], columns[i, :, 17] = unit(i * m, 384)
        columns[i, :, 18], columns[i, :, 19] = unit(i * (m + 256), 384)
    re, im = unit(m[:, None] * np.arange(8)[None, :], 1024)
    columns[3, :, 0:8], columns[3, :, 8:16] = re, im
    inner = np.stack(unit(m[:, None] * lane[None, :], B)).astype(np.float32)
    outer = np.stack(unit(np.arange(8)[:, None] * lane[None, :], 1024)).astype(np.float32)
    return high, low, lanes, place, columns, inner, outer


def split(value):
    high = value.astype(BF16)
    return high, (value - high.astype(F32)).astype(BF16)


def from_left(high, low, value):
    left = jnp.concatenate([high, high, low], axis=1)
    top, rest = split(value)
    right = jnp.concatenate([top, rest, top], axis=0)
    return jnp.dot(left, right, preferred_element_type=F32)


def from_right(value, high, low):
    top, rest = split(value)
    left = jnp.concatenate([top, rest, top], axis=1)
    right = jnp.concatenate([high, high, low], axis=0)
    return jnp.dot(left, right, preferred_element_type=F32)


def times(a, b):
    return a[0] * b[0] - a[1] * b[1], a[0] * b[1] + a[1] * b[0]


def times_conj(a, b):
    return a[0] * b[0] + a[1] * b[1], a[1] * b[0] - a[0] * b[1]


def turn(a, sign):
    return (-a[1], a[0]) if sign > 0 else (a[1], -a[0])


def add(a, b):
    return a[0] + b[0], a[1] + b[1]


def sub(a, b):
    return a[0] - b[0], a[1] - b[1]


def four(a, b, c, d, sign):
    even, odd = add(a, c), sub(a, c)
    other, cross = add(b, d), turn(sub(b, d), sign)
    return add(even, other), add(odd, cross), sub(even, other), sub(odd, cross)


def eight(v, sign):
    even = four(v[0], v[2], v[4], v[6], sign)
    odd = four(v[1], v[3], v[5], v[7], sign)
    half = math.sqrt(0.5)
    one = turn(odd[1], sign)
    one = ((odd[1][0] + one[0]) * half, (odd[1][1] + one[1]) * half)
    two = turn(odd[2], sign)
    three = turn(odd[3], sign)
    three = ((three[0] - odd[3][0]) * half, (three[1] - odd[3][1]) * half)
    odd = (odd[0], one, two, three)
    return [add(e, o) for e, o in zip(even, odd)] + [sub(e, o) for e, o in zip(even, odd)]


def paired(first, second):
    re = jnp.concatenate([first[0], second[0]], axis=1)
    im = jnp.concatenate([first[1], second[1]], axis=1)
    return jnp.concatenate([re, im], axis=0)


def parts(value, which):
    cols = slice(128 * which, 128 * which + 128)
    return value[:128, cols], value[128:, cols]


def kernel(
    x,
    high,
    low,
    lanes,
    place,
    columns,
    inner,
    outer,
    out,
    kept,
    sent,
    field,
    back,
    home,
    final,
    total,
    work,
    turn1,
    turn2,
    turn3,
    start,
    send,
    recv,
):
    row = lax.axis_index("row")
    col = lax.axis_index("col")
    me = row * 16 + col

    def peer(step):
        t = (step * STEP) % 128
        to_row = ((row // 2 + t // 32) % 4) * 2 + (row % 2 + (t // 16) % 2) % 2
        to_col = ((col // 4 + (t // 4) % 4) % 4) * 4 + (col % 4 + t % 4) % 4
        return to_row, to_col, to_row * 16 + to_col

    barrier = pltpu.get_barrier_semaphore()

    def greet(step, carry):
        to_row, to_col, _ = peer(step)
        pl.semaphore_signal(barrier, inc=1, device_id=(to_row, to_col), device_id_type=MESH)
        return carry

    lax.fori_loop(1, DEVICES, greet, 0)
    pl.semaphore_wait(barrier, DEVICES - 1)

    def exchange(src_of, dst_of, phase):
        pltpu.make_async_copy(src_of(me), dst_of(me), recv.at[phase]).start()

        def one(step, carry):
            to_row, to_col, to = peer(step)
            pltpu.make_async_remote_copy(
                src_ref=src_of(to),
                dst_ref=dst_of(me),
                send_sem=send.at[phase],
                recv_sem=recv.at[phase],
                device_id=(to_row, to_col),
                device_id_type=MESH,
            ).start()
            return carry

        lax.fori_loop(1, DEVICES, one, 0)

    def arrived(ref, phase):
        pltpu.make_async_copy(ref, ref, recv.at[phase]).wait()

    def gone(ref, phase):
        pltpu.make_async_copy(ref, ref, send.at[phase]).wait()

    exchange(lambda q: x.at[:, q], lambda p: kept.at[pl.ds(2 * p, 2)], 0)

    here = lax.broadcasted_iota(jnp.int32, (128, 128), 1) == me

    def prepare(i, carry):
        own = [
            jnp.sum(jnp.where(here, place[i, r], 0.0), axis=1, keepdims=True) for r in range(2)
        ]
        base = lanes[i, 0], lanes[i, 1]
        for c in range(8):
            step = columns[i, :, c : c + 1], columns[i, :, 8 + c : 9 + c]
            re, im = times(times(own, step), base)
            turn1[i, c, 0], turn1[i, c, 1] = re, im
        for k in range(4):
            start[i, k] = jnp.broadcast_to(columns[i, :, 16 + k : 17 + k], (128, 128))
        return carry

    lax.fori_loop(0, 3, prepare, 0)
    for s in range(8):
        for r in range(2):
            turn2[s, r] = jnp.broadcast_to(columns[3, :, 8 * r + s : 8 * r + s + 1], (128, 128))
        re, im = times((inner[0], inner[1]), (outer[0, s : s + 1], outer[1, s : s + 1]))
        turn3[s, 0], turn3[s, 1] = re, im
    total[...] = jnp.zeros_like(total)

    kept_rows = kept.reshape(4096, 128)
    sent_rows = sent.reshape(3, 2048, 128)
    field_rows = field.reshape(3, 2, 1024, 128)
    back_rows = back.reshape(3, 2048, 128)
    home_rows = home.reshape(3, 2048, 128)
    final_rows = final.reshape(4096, 128)

    def every(first, gap):
        return pl.ds(first, 128, stride=gap)

    arrived(kept, 0)

    def expand(i, carry):
        by_low = start[i, 0], start[i, 1]
        by_high = start[i, 2], start[i, 3]
        for g in range(4):
            pair = []
            for c in (2 * g, 2 * g + 1):
                below = kept_rows[every(2 * c, 16), :], kept_rows[every(2 * c + 1, 16), :]
                above = (
                    kept_rows[every(2048 + 2 * c, 16), :],
                    kept_rows[every(2049 + 2 * c, 16), :],
                )
                pair.append(add(times(below, by_low), times(above, by_high)))
            mixed = from_left(high[0], low[0], paired(*pair))
            for w in range(2):
                c = 2 * g + w
                re, im = times(parts(mixed, w), (turn1[i, c, 0], turn1[i, c, 1]))
                sent_rows[i, every(c, 16), :] = re
                sent_rows[i, every(8 + c, 16), :] = im
        exchange(lambda q: sent.at[i, q], lambda p: field.at[i, :, p], 1 + i)
        return carry

    lax.fori_loop(0, 3, expand, 0)

    scale = 1.0 / math.sqrt(MODES)
    factor = 1.0 / math.sqrt(POINTS)

    def middle(i, carry):
        arrived(field.at[i], 1 + i)
        for g in range(4):
            pair = [
                (field_rows[i, 0, every(s, 8), :], field_rows[i, 1, every(s, 8), :])
                for s in (2 * g, 2 * g + 1)
            ]
            mixed = from_left(high[0], low[0], paired(*pair))
            for w in range(2):
                work[2 * g + w, 0], work[2 * g + w, 1] = parts(mixed, w)

        def rise(k, inside):
            rows = pl.ds(pl.multiple_of(8 * k, 8), 8)
            v = [
                times(
                    (work[s, 0, rows, :], work[s, 1, rows, :]),
                    (turn2[s, 0, rows, :], turn2[s, 1, rows, :]),
                )
                for s in range(8)
            ]
            v = eight(v, 1)
            for s in range(8):
                re, im = times(v[s], (turn3[s, 0, rows, :], turn3[s, 1, rows, :]))
                work[s, 0, rows, :] = re
                work[s, 1, rows, :] = im
            return inside

        lax.fori_loop(0, 16, rise, 0)

        def peak(k, inside):
            some = pl.ds(4 * k, 4)
            value = jnp.concatenate(
                [work[some, 0].reshape(512, 128), work[some, 1].reshape(512, 128)], axis=1
            )
            value = from_right(value, high[1], low[1]) * scale
            re, im = value[:, :128], value[:, 128:]
            value = jnp.concatenate(
                [(re * re - im * im) * factor, (2.0 * factor) * (re * im)], axis=1
            )
            value = from_right(value, high[0], low[0])
            re, im = times_conj(
                (value[:, :128].reshape(4, 128, 128), value[:, 128:].reshape(4, 128, 128)),
                (turn3[some, 0], turn3[some, 1]),
            )
            work[some, 0] = re
            work[some, 1] = im
            return inside

        lax.fori_loop(0, 2, peak, 0)

        def fall(k, inside):
            rows = pl.ds(pl.multiple_of(8 * k, 8), 8)
            v = eight([(work[s, 0, rows, :], work[s, 1, rows, :]) for s in range(8)], -1)
            for s in range(8):
                re, im = times_conj(v[s], (turn2[s, 0, rows, :], turn2[s, 1, rows, :]))
                work[s, 0, rows, :] = re
                work[s, 1, rows, :] = im
            return inside

        lax.fori_loop(0, 16, fall, 0)
        for g in range(4):
            pair = [(work[s, 0], work[s, 1]) for s in (2 * g, 2 * g + 1)]
            mixed = from_left(high[1], low[1], paired(*pair))
            for w in range(2):
                s = 2 * g + w
                re, im = parts(mixed, w)
                back_rows[i, every(s, 16), :] = re
                back_rows[i, every(8 + s, 16), :] = im
        exchange(lambda q: back.at[i, q], lambda p: home.at[i, p], 4 + i)
        return carry

    lax.fori_loop(0, 3, middle, 0)

    def gather(i, carry):
        arrived(home.at[i], 4 + i)
        by_low = start[i, 0], start[i, 1]
        by_high = start[i, 2], start[i, 3]
        for g in range(4):
            pair = [
                times_conj(
                    (home_rows[i, every(c, 16), :], home_rows[i, every(8 + c, 16), :]),
                    (turn1[i, c, 0], turn1[i, c, 1]),
                )
                for c in (2 * g, 2 * g + 1)
            ]
            mixed = from_left(high[1], low[1], paired(*pair))
            for w in range(2):
                c = 2 * g + w
                value = parts(mixed, w)
                for h, by in enumerate((by_low, by_high)):
                    re, im = times_conj(value, by)
                    total[c, h, 0] += re
                    total[c, h, 1] += im
        return carry

    lax.fori_loop(0, 3, gather, 0)
    for c in range(8):
        for h in range(2):
            for r in range(2):
                final_rows[every(2048 * h + 2 * c + r, 16), :] = total[c, h, r]
    exchange(lambda q: final.at[pl.ds(2 * q, 2)], lambda p: out.at[:, p], 7)
    others = pl.ds(0, DEVICES - 1)
    gone(x.at[:, others], 0)
    for i in range(3):
        gone(sent.at[i, others], 1 + i)
        gone(back.at[i, others], 4 + i)
    arrived(out, 7)
    gone(final.at[pl.ds(0, 2 * (DEVICES - 1))], 7)


def body(spectrum):
    x = spectrum.reshape(2, 2048, 128).transpose(1, 0, 2).reshape(2, 128, 16, 128)
    vmem = pl.BlockSpec(memory_space=pltpu.VMEM)
    anywhere = pl.BlockSpec(memory_space=pl.ANY)
    out = pl.pallas_call(
        kernel,
        name="convolve",
        out_shape=jax.ShapeDtypeStruct((2, 128, 16, 128), F32),
        in_specs=[anywhere] + [vmem] * 7,
        out_specs=anywhere,
        scratch_shapes=[
            pltpu.VMEM((256, 16, 128), F32),
            pltpu.VMEM((3, 128, 2, 8, 128), F32),
            pltpu.VMEM((3, 2, 128, 8, 128), F32),
            pltpu.VMEM((3, 128, 2, 8, 128), F32),
            pltpu.VMEM((3, 128, 2, 8, 128), F32),
            pltpu.VMEM((256, 16, 128), F32),
            pltpu.VMEM((8, 2, 2, 128, 128), F32),
            pltpu.VMEM((8, 2, 128, 128), F32),
            pltpu.VMEM((3, 8, 2, 128, 128), F32),
            pltpu.VMEM((8, 2, 128, 128), F32),
            pltpu.VMEM((8, 2, 128, 128), F32),
            pltpu.VMEM((3, 4, 128, 128), F32),
            pltpu.SemaphoreType.DMA((8,)),
            pltpu.SemaphoreType.DMA((8,)),
        ],
        compiler_params=pltpu.CompilerParams(
            collective_id=0, has_side_effects=True, vmem_limit_bytes=56 * 1024 * 1024
        ),
    )(x, *[jnp.asarray(t) for t in tables()])
    return out.reshape(2048, 2, 128).transpose(1, 0, 2).reshape(2, 262144)


def solution(mesh):
    return jax.shard_map(
        body,
        mesh=mesh,
        in_specs=(P(None, ("row", "col")),),
        out_specs=P(None, ("row", "col")),
        check_vma=False,
    )
```

```python
import functools
import math

import jax
import jax.numpy as jnp
import numpy as np
from jax import lax
from jax.experimental import pallas as pl
from jax.experimental.pallas import tpu as pltpu
from jax.sharding import PartitionSpec as P

B = 131072
MODES = 33554432
POINTS = 50331648
DEVICES = 128
STEP = 37

MESH = pl.DeviceIdType.MESH
F32 = jnp.float32
BF16 = jnp.bfloat16


def unit(turns, total):
    angle = 2.0 * np.pi * (np.asarray(turns, np.int64) % total) / total
    return np.cos(angle), np.sin(angle)


def tables():
    m = np.arange(128)
    lane = np.arange(128)
    cos, sin = unit(m[:, None] * m[None, :], 128)
    plus = np.block([[cos, -sin], [sin, cos]])
    both = np.stack([plus, plus.T]).astype(np.float32)
    high = both.astype(BF16)
    low = (both - high.astype(np.float32)).astype(BF16)
    lanes = np.zeros((3, 2, 128, 128), np.float32)
    place = np.zeros((3, 2, 128, 128), np.float32)
    columns = np.zeros((4, 128, 128), np.float32)
    for i in range(3):
        mine = i + 3 * m
        lanes[i] = unit(mine[:, None] * lane[None, :], POINTS)
        place[i] = unit(mine[:, None] * lane[None, :] * 1024, POINTS)
        re, im = unit(mine[:, None] * np.arange(8)[None, :] * 128, POINTS)
        columns[i, :, 0:8], columns[i, :, 8:16] = re, im
        columns[i, :, 16], columns[i, :, 17] = unit(i * m, 384)
        columns[i, :, 18], columns[i, :, 19] = unit(i * (m + 256), 384)
    re, im = unit(m[:, None] * np.arange(8)[None, :], 1024)
    columns[3, :, 0:8], columns[3, :, 8:16] = re, im
    inner = np.stack(unit(m[:, None] * lane[None, :], B)).astype(np.float32)
    outer = np.stack(unit(np.arange(8)[:, None] * lane[None, :], 1024)).astype(np.float32)
    return high, low, lanes, place, columns, inner, outer


def split(value):
    high = value.astype(BF16)
    return high, (value - high.astype(F32)).astype(BF16)


def from_left(high, low, value):
    left = jnp.concatenate([high, high, low], axis=1)
    top, rest = split(value)
    right = jnp.concatenate([top, rest, top], axis=0)
    return jnp.dot(left, right, preferred_element_type=F32)


def from_right(value, high, low):
    top, rest = split(value)
    left = jnp.concatenate([top, rest, top], axis=1)
    right = jnp.concatenate([high, high, low], axis=0)
    return jnp.dot(left, right, preferred_element_type=F32)


def times(a, b):
    return a[0] * b[0] - a[1] * b[1], a[0] * b[1] + a[1] * b[0]


def times_conj(a, b):
    return a[0] * b[0] + a[1] * b[1], a[1] * b[0] - a[0] * b[1]


def turn(a, sign):
    return (-a[1], a[0]) if sign > 0 else (a[1], -a[0])


def add(a, b):
    return a[0] + b[0], a[1] + b[1]


def sub(a, b):
    return a[0] - b[0], a[1] - b[1]


def four(a, b, c, d, sign):
    even, odd = add(a, c), sub(a, c)
    other, cross = add(b, d), turn(sub(b, d), sign)
    return add(even, other), add(odd, cross), sub(even, other), sub(odd, cross)


def eight(v, sign):
    even = four(v[0], v[2], v[4], v[6], sign)
    odd = four(v[1], v[3], v[5], v[7], sign)
    half = math.sqrt(0.5)
    one = turn(odd[1], sign)
    one = ((odd[1][0] + one[0]) * half, (odd[1][1] + one[1]) * half)
    two = turn(odd[2], sign)
    three = turn(odd[3], sign)
    three = ((three[0] - odd[3][0]) * half, (three[1] - odd[3][1]) * half)
    odd = (odd[0], one, two, three)
    return [add(e, o) for e, o in zip(even, odd)] + [sub(e, o) for e, o in zip(even, odd)]


def paired(first, second):
    re = jnp.concatenate([first[0], second[0]], axis=1)
    im = jnp.concatenate([first[1], second[1]], axis=1)
    return jnp.concatenate([re, im], axis=0)


def parts(value, which):
    cols = slice(128 * which, 128 * which + 128)
    return value[:128, cols], value[128:, cols]


def wrap(value, size):
    return jnp.where(value >= size, value - size, value)


def kernel(
    x_far,
    high_far,
    low_far,
    lanes_far,
    place_far,
    columns_far,
    inner_far,
    outer_far,
    out,
    x,
    high,
    low,
    lanes,
    place,
    columns,
    inner,
    outer,
    kept,
    sent,
    field,
    back,
    home,
    final,
    total,
    work,
    turn1,
    turn2,
    turn3,
    start,
    load,
    send,
    recv,
):
    row = lax.axis_index("row")
    col = lax.axis_index("col")
    me = row * 16 + col

    loads = [
        pltpu.make_async_copy(far, near, load.at[k])
        for k, (far, near) in enumerate(
            (
                (x_far, x),
                (high_far, high),
                (low_far, low),
                (lanes_far, lanes),
                (place_far, place),
                (columns_far, columns),
                (inner_far, inner),
                (outer_far, outer),
            )
        )
    ]
    for one in loads:
        one.start()

    cols = [wrap(col + c, 16) for c in range(16)]

    def each_peer(act):
        def group(o, base):
            rows = [wrap(base + k, 8) for k in range(8)]
            for u in range(16):
                to_row, to_col = rows[(STEP * u // 16) % 8], cols[STEP * u % 16]
                if u == 0:
                    pl.when(o > 0)(functools.partial(act, to_row, to_col))
                else:
                    act(to_row, to_col)
            return wrap(base + STEP % 8, 8)

        lax.fori_loop(0, 8, group, row)

    barrier = pltpu.get_barrier_semaphore()

    def greet(to_row, to_col):
        pl.semaphore_signal(barrier, inc=1, device_id=(to_row, to_col), device_id_type=MESH)

    each_peer(greet)
    loads[0].wait()
    pl.semaphore_wait(barrier, DEVICES - 1)

    def exchange(src_of, dst_of, phase):
        mine = dst_of(me)

        def one(to_row, to_col):
            pltpu.make_async_remote_copy(
                src_ref=src_of(to_row * 16 + to_col),
                dst_ref=mine,
                send_sem=send.at[phase],
                recv_sem=recv.at[phase],
                device_id=(to_row, to_col),
                device_id_type=MESH,
            ).start()

        each_peer(one)
        pltpu.make_async_copy(src_of(me), mine, recv.at[phase]).start()

    def arrived(ref, phase):
        pltpu.make_async_copy(ref, ref, recv.at[phase]).wait()

    def gone(ref, phase):
        pltpu.make_async_copy(ref, ref, send.at[phase]).wait()

    def first(h, carry):
        some = pl.ds(pl.multiple_of(8 * h, 8), 8)
        exchange(lambda q: x.at[:, q, some], lambda p: kept.at[h, pl.ds(2 * p, 2)], h)
        return carry

    lax.fori_loop(0, 2, first, 0)
    for one in loads[1:]:
        one.wait()

    here = lax.broadcasted_iota(jnp.int32, (128, 128), 1) == me

    def prepare(i, carry):
        own = [
            jnp.sum(jnp.where(here, place[i, r], 0.0), axis=1, keepdims=True) for r in range(2)
        ]
        base = lanes[i, 0], lanes[i, 1]
        for c in range(8):
            step = columns[i, :, c : c + 1], columns[i, :, 8 + c : 9 + c]
            re, im = times(times(own, step), base)
            turn1[i, c, 0], turn1[i, c, 1] = re, im
        for k in range(4):
            start[i, k] = jnp.broadcast_to(columns[i, :, 16 + k : 17 + k], (128, 128))
        return carry

    lax.fori_loop(0, 3, prepare, 0)
    for s in range(8):
        for r in range(2):
            turn2[s, r] = jnp.broadcast_to(columns[3, :, 8 * r + s : 8 * r + s + 1], (128, 128))
        re, im = times((inner[0], inner[1]), (outer[0, s : s + 1], outer[1, s : s + 1]))
        turn3[s, 0], turn3[s, 1] = re, im
    total[...] = jnp.zeros_like(total)

    kept_rows = kept.reshape(2, 2048, 128)
    sent_rows = sent.reshape(3, 2, 1024, 128)
    field_rows = field.reshape(3, 2, 1024, 128)
    back_rows = back.reshape(3, 2, 1024, 128)
    home_rows = home.reshape(3, 2, 1024, 128)
    final_rows = final.reshape(2, 2048, 128)

    def every(first_row):
        return pl.ds(first_row, 128, stride=8)

    def expand(j, carry):
        i, h = lax.div(j, 2), lax.rem(j, 2)

        @pl.when(j < 2)
        def _():
            arrived(kept.at[h], h)

        by_low = start[i, 0], start[i, 1]
        by_high = start[i, 2], start[i, 3]
        for g in range(2):
            pair = []
            for c in (2 * g, 2 * g + 1):
                below = kept_rows[h, every(2 * c), :], kept_rows[h, every(2 * c + 1), :]
                above = (
                    kept_rows[h, every(1024 + 2 * c), :],
                    kept_rows[h, every(1025 + 2 * c), :],
                )
                pair.append(add(times(below, by_low), times(above, by_high)))
            mixed = from_left(high[0], low[0], paired(*pair))
            for w in range(2):
                c = 2 * g + w
                by = turn1[i, 4 * h + c, 0], turn1[i, 4 * h + c, 1]
                re, im = times(parts(mixed, w), by)
                sent_rows[i, h, every(c), :] = re
                sent_rows[i, h, every(4 + c), :] = im
        exchange(lambda q: sent.at[i, h, q], lambda p: field.at[i, h, p], 2 + j)
        return carry

    lax.fori_loop(0, 6, expand, 0)

    scale = 1.0 / math.sqrt(MODES)

    def middle(i, carry):
        for h in range(2):
            arrived(field.at[i, h], 2 + 2 * i + h)
            for g in range(2):
                pair = [
                    (field_rows[i, h, every(s), :], field_rows[i, h, every(4 + s), :])
                    for s in (2 * g, 2 * g + 1)
                ]
                mixed = from_left(high[0], low[0], paired(*pair))
                for w in range(2):
                    s = 4 * h + 2 * g + w
                    work[s, 0], work[s, 1] = parts(mixed, w)

        def rise(k, inside):
            rows = pl.ds(pl.multiple_of(8 * k, 8), 8)
            v = [
                times(
                    (work[s, 0, rows, :], work[s, 1, rows, :]),
                    (turn2[s, 0, rows, :], turn2[s, 1, rows, :]),
                )
                for s in range(8)
            ]
            v = eight(v, 1)
            for s in range(8):
                re, im = times(v[s], (turn3[s, 0, rows, :], turn3[s, 1, rows, :]))
                work[s, 0, rows, :] = re
                work[s, 1, rows, :] = im
            return inside

        lax.fori_loop(0, 16, rise, 0)

        def peak(k, inside):
            some = pl.ds(4 * k, 4)
            value = jnp.concatenate(
                [work[some, 0].reshape(512, 128), work[some, 1].reshape(512, 128)], axis=1
            )
            value = from_right(value, high[1], low[1]) * scale
            re, im = value[:, :128], value[:, 128:]
            value = jnp.concatenate([re * re - im * im, 2.0 * (re * im)], axis=1)
            value = from_right(value, high[0], low[0])
            re, im = times_conj(
                (value[:, :128].reshape(4, 128, 128), value[:, 128:].reshape(4, 128, 128)),
                (turn3[some, 0], turn3[some, 1]),
            )
            work[some, 0] = re
            work[some, 1] = im
            return inside

        lax.fori_loop(0, 2, peak, 0)

        def fall(k, inside):
            rows = pl.ds(pl.multiple_of(8 * k, 8), 8)
            v = eight([(work[s, 0, rows, :], work[s, 1, rows, :]) for s in range(8)], -1)
            for s in range(8):
                re, im = times_conj(v[s], (turn2[s, 0, rows, :], turn2[s, 1, rows, :]))
                work[s, 0, rows, :] = re
                work[s, 1, rows, :] = im
            return inside

        lax.fori_loop(0, 16, fall, 0)

        def part(h, inside):
            for g in range(2):
                pair = [(work[4 * h + s, 0], work[4 * h + s, 1]) for s in (2 * g, 2 * g + 1)]
                mixed = from_left(high[1], low[1], paired(*pair))
                for w in range(2):
                    s = 2 * g + w
                    re, im = parts(mixed, w)
                    back_rows[i, h, every(s), :] = re
                    back_rows[i, h, every(4 + s), :] = im
            exchange(lambda q: back.at[i, h, q], lambda p: home.at[i, h, p], 8 + 2 * i + h)
            return inside

        lax.fori_loop(0, 2, part, 0)
        return carry

    lax.fori_loop(0, 3, middle, 0)

    def gather(j, carry):
        i, h = lax.div(j, 2), lax.rem(j, 2)
        arrived(home.at[i, h], 8 + j)
        by_low = start[i, 0], start[i, 1]
        by_high = start[i, 2], start[i, 3]
        for g in range(2):
            pair = [
                times_conj(
                    (home_rows[i, h, every(c), :], home_rows[i, h, every(4 + c), :]),
                    (turn1[i, 4 * h + c, 0], turn1[i, 4 * h + c, 1]),
                )
                for c in (2 * g, 2 * g + 1)
            ]
            mixed = from_left(high[1], low[1], paired(*pair))
            for w in range(2):
                c = 2 * g + w
                value = parts(mixed, w)
                for f, by in enumerate((by_low, by_high)):
                    re, im = times_conj(value, by)
                    total[h, c, f, 0] += re
                    total[h, c, f, 1] += im

        @pl.when(i == 2)
        def _():
            for c in range(4):
                for f in range(2):
                    for r in range(2):
                        final_rows[h, every(1024 * f + 2 * c + r), :] = total[h, c, f, r]
            some = pl.ds(pl.multiple_of(8 * h, 8), 8)
            exchange(
                lambda q: final.at[h, pl.ds(2 * q, 2)], lambda p: out.at[:, p, some], 14 + h
            )

        return carry

    lax.fori_loop(0, 6, gather, 0)
    others = pl.ds(0, DEVICES - 1)
    double = pl.ds(0, 2 * (DEVICES - 1))
    for h in range(2):
        gone(kept.at[h, double], h)
        for i in range(3):
            gone(sent.at[i, h, others], 2 + 2 * i + h)
            gone(back.at[i, h, others], 8 + 2 * i + h)
    for h in range(2):
        arrived(final.at[h], 14 + h)
        gone(final.at[h, double], 14 + h)


def body(spectrum):
    x = spectrum.reshape(2, 2048, 128).transpose(1, 0, 2).reshape(2, 128, 16, 128)
    anywhere = pl.BlockSpec(memory_space=pl.ANY)
    held = [jnp.asarray(t) for t in tables()]
    grid = (3, 2, 128, 8, 128)
    out = pl.pallas_call(
        kernel,
        name="convolve",
        out_shape=jax.ShapeDtypeStruct((2, 128, 16, 128), F32),
        in_specs=[anywhere] * (1 + len(held)),
        out_specs=anywhere,
        scratch_shapes=[
            pltpu.VMEM((2, 128, 16, 128), F32),
            *[pltpu.VMEM(t.shape, t.dtype) for t in held],
            pltpu.VMEM((2, 256, 8, 128), F32),
            pltpu.VMEM(grid, F32),
            pltpu.VMEM(grid, F32),
            pltpu.VMEM(grid, F32),
            pltpu.VMEM(grid, F32),
            pltpu.VMEM((2, 256, 8, 128), F32),
            pltpu.VMEM((2, 4, 2, 2, 128, 128), F32),
            pltpu.VMEM((8, 2, 128, 128), F32),
            pltpu.VMEM((3, 8, 2, 128, 128), F32),
            pltpu.VMEM((8, 2, 128, 128), F32),
            pltpu.VMEM((8, 2, 128, 128), F32),
            pltpu.VMEM((3, 4, 128, 128), F32),
            pltpu.SemaphoreType.DMA((8,)),
            pltpu.SemaphoreType.DMA((16,)),
            pltpu.SemaphoreType.DMA((16,)),
        ],
        compiler_params=pltpu.CompilerParams(
            collective_id=0, has_side_effects=True, vmem_limit_bytes=56 * 1024 * 1024
        ),
    )(x, *held)
    out = out * F32(1.0 / math.sqrt(POINTS))
    return out.reshape(2048, 2, 128).transpose(1, 0, 2).reshape(2, 262144)


def solution(mesh):
    return jax.shard_map(
        body,
        mesh=mesh,
        in_specs=(P(None, ("row", "col")),),
        out_specs=P(None, ("row", "col")),
        check_vma=False,
    )
```

```python
import functools
import math

import jax
import jax.numpy as jnp
import numpy as np
from jax import lax
from jax.experimental import pallas as pl
from jax.experimental.pallas import tpu as pltpu
from jax.sharding import PartitionSpec as P

B = 131072
MODES = 33554432
POINTS = 50331648
DEVICES = 128
STEP = 37


def far_to_near():
    hops = [0, 1, 2, 1]
    steps = [(STEP * k) % 128 for k in range(1, DEVICES)]
    steps = [(t // 32, t // 16 % 2, t // 4 % 4, t % 4) for t in steps]
    return sorted(steps, key=lambda t: -(hops[t[0]] + hops[t[2]] + hops[t[3]]))


FAR = far_to_near()

MESH = pl.DeviceIdType.MESH
F32 = jnp.float32
BF16 = jnp.bfloat16


def unit(turns, total):
    angle = 2.0 * np.pi * (np.asarray(turns, np.int64) % total) / total
    return np.cos(angle), np.sin(angle)


def tables():
    m = np.arange(128)
    lane = np.arange(128)
    cos, sin = unit(m[:, None] * m[None, :], 128)
    plus = np.block([[cos, -sin], [sin, cos]])
    both = np.stack([plus, plus.T]).astype(np.float32)
    high = both.astype(BF16)
    low = (both - high.astype(np.float32)).astype(BF16)
    lanes = np.zeros((3, 2, 128, 128), np.float32)
    place = np.zeros((3, 2, 128, 128), np.float32)
    columns = np.zeros((4, 128, 128), np.float32)
    for i in range(3):
        mine = i + 3 * m
        lanes[i] = unit(mine[:, None] * lane[None, :], POINTS)
        place[i] = unit(mine[:, None] * lane[None, :] * 1024, POINTS)
        re, im = unit(mine[:, None] * np.arange(8)[None, :] * 128, POINTS)
        columns[i, :, 0:8], columns[i, :, 8:16] = re, im
        columns[i, :, 16], columns[i, :, 17] = unit(i * m, 384)
        columns[i, :, 18], columns[i, :, 19] = unit(i * (m + 256), 384)
    re, im = unit(m[:, None] * np.arange(8)[None, :], 1024)
    columns[3, :, 0:8], columns[3, :, 8:16] = re, im
    inner = np.stack(unit(m[:, None] * lane[None, :], B)).astype(np.float32)
    outer = np.stack(unit(np.arange(8)[:, None] * lane[None, :], 1024)).astype(np.float32)
    return high, low, lanes, place, columns, inner, outer


def split(value):
    high = value.astype(BF16)
    return high, (value - high.astype(F32)).astype(BF16)


def from_left(high, low, value):
    left = jnp.concatenate([high, high, low], axis=1)
    top, rest = split(value)
    right = jnp.concatenate([top, rest, top], axis=0)
    return jnp.dot(left, right, preferred_element_type=F32)


def from_right(value, high, low):
    top, rest = split(value)
    left = jnp.concatenate([top, rest, top], axis=1)
    right = jnp.concatenate([high, high, low], axis=0)
    return jnp.dot(left, right, preferred_element_type=F32)


def times(a, b):
    return a[0] * b[0] - a[1] * b[1], a[0] * b[1] + a[1] * b[0]


def times_conj(a, b):
    return a[0] * b[0] + a[1] * b[1], a[1] * b[0] - a[0] * b[1]


def turn(a, sign):
    return (-a[1], a[0]) if sign > 0 else (a[1], -a[0])


def add(a, b):
    return a[0] + b[0], a[1] + b[1]


def sub(a, b):
    return a[0] - b[0], a[1] - b[1]


def four(a, b, c, d, sign):
    even, odd = add(a, c), sub(a, c)
    other, cross = add(b, d), turn(sub(b, d), sign)
    return add(even, other), add(odd, cross), sub(even, other), sub(odd, cross)


def eight(v, sign):
    even = four(v[0], v[2], v[4], v[6], sign)
    odd = four(v[1], v[3], v[5], v[7], sign)
    half = math.sqrt(0.5)
    one = turn(odd[1], sign)
    one = ((odd[1][0] + one[0]) * half, (odd[1][1] + one[1]) * half)
    two = turn(odd[2], sign)
    three = turn(odd[3], sign)
    three = ((three[0] - odd[3][0]) * half, (three[1] - odd[3][1]) * half)
    odd = (odd[0], one, two, three)
    return [add(e, o) for e, o in zip(even, odd)] + [sub(e, o) for e, o in zip(even, odd)]


def paired(first, second):
    re = jnp.concatenate([first[0], second[0]], axis=1)
    im = jnp.concatenate([first[1], second[1]], axis=1)
    return jnp.concatenate([re, im], axis=0)


def parts(value, which):
    cols = slice(128 * which, 128 * which + 128)
    return value[:128, cols], value[128:, cols]


def wrap(value, size):
    return jnp.where(value >= size, value - size, value)


def kernel(
    x_far,
    high_far,
    low_far,
    lanes_far,
    place_far,
    columns_far,
    inner_far,
    outer_far,
    out,
    x,
    high,
    low,
    lanes,
    place,
    columns,
    inner,
    outer,
    kept,
    sent,
    field,
    back,
    home,
    final,
    total,
    work,
    turn1,
    turn2,
    turn3,
    start,
    load,
    send,
    recv,
):
    row = lax.axis_index("row")
    col = lax.axis_index("col")
    me = row * 16 + col

    loads = [
        pltpu.make_async_copy(far, near, load.at[k])
        for k, (far, near) in enumerate(
            (
                (x_far, x),
                (high_far, high),
                (low_far, low),
                (lanes_far, lanes),
                (place_far, place),
                (columns_far, columns),
                (inner_far, inner),
                (outer_far, outer),
            )
        )
    ]
    for one in loads:
        one.start()

    cols = [wrap(col + c, 16) for c in range(16)]

    def each_peer(act):
        def group(o, base):
            rows = [wrap(base + k, 8) for k in range(8)]
            for u in range(16):
                to_row, to_col = rows[(STEP * u // 16) % 8], cols[STEP * u % 16]
                if u == 0:
                    pl.when(o > 0)(functools.partial(act, to_row, to_col))
                else:
                    act(to_row, to_col)
            return wrap(base + STEP % 8, 8)

        lax.fori_loop(0, 8, group, row)

    at_x, at_core = lax.div(row, 2), lax.rem(row, 2)
    at_z, at_y = lax.div(col, 4), lax.rem(col, 4)
    to_x = [wrap(at_x + d, 4) * 2 for d in range(4)]
    to_core = [wrap(at_core + d, 2) for d in range(2)]
    to_z = [wrap(at_z + d, 4) * 4 for d in range(4)]
    to_y = [wrap(at_y + d, 4) for d in range(4)]

    def far_first(act):
        for dx, dc, dz, dy in FAR:
            act(to_x[dx] + to_core[dc], to_z[dz] + to_y[dy])

    barrier = pltpu.get_barrier_semaphore()

    def greet(to_row, to_col):
        pl.semaphore_signal(barrier, inc=1, device_id=(to_row, to_col), device_id_type=MESH)

    far_first(greet)
    loads[0].wait()
    pl.semaphore_wait(barrier, DEVICES - 1)

    def exchange(src_of, dst_of, phase, order=each_peer):
        mine = dst_of(me)

        def one(to_row, to_col):
            pltpu.make_async_remote_copy(
                src_ref=src_of(to_row * 16 + to_col),
                dst_ref=mine,
                send_sem=send.at[phase],
                recv_sem=recv.at[phase],
                device_id=(to_row, to_col),
                device_id_type=MESH,
            ).start()

        order(one)
        pltpu.make_async_copy(src_of(me), mine, recv.at[phase]).start()

    def arrived(ref, phase):
        pltpu.make_async_copy(ref, ref, recv.at[phase]).wait()

    def gone(ref, phase):
        pltpu.make_async_copy(ref, ref, send.at[phase]).wait()

    def first(h, carry):
        some = pl.ds(pl.multiple_of(8 * h, 8), 8)
        exchange(lambda q: x.at[:, q, some], lambda p: kept.at[h, pl.ds(2 * p, 2)], h)
        return carry

    lax.fori_loop(0, 2, first, 0)
    for one in loads[1:]:
        one.wait()

    here = lax.broadcasted_iota(jnp.int32, (128, 128), 1) == me

    def prepare(i, carry):
        own = [
            jnp.sum(jnp.where(here, place[i, r], 0.0), axis=1, keepdims=True) for r in range(2)
        ]
        base = lanes[i, 0], lanes[i, 1]
        for c in range(8):
            step = columns[i, :, c : c + 1], columns[i, :, 8 + c : 9 + c]
            re, im = times(times(own, step), base)
            turn1[i, c, 0], turn1[i, c, 1] = re, im
        for k in range(4):
            start[i, k] = jnp.broadcast_to(columns[i, :, 16 + k : 17 + k], (128, 128))
        return carry

    lax.fori_loop(0, 3, prepare, 0)
    for s in range(8):
        for r in range(2):
            turn2[s, r] = jnp.broadcast_to(columns[3, :, 8 * r + s : 8 * r + s + 1], (128, 128))
        re, im = times((inner[0], inner[1]), (outer[0, s : s + 1], outer[1, s : s + 1]))
        turn3[s, 0], turn3[s, 1] = re, im
    total[...] = jnp.zeros_like(total)

    kept_rows = kept.reshape(2, 2048, 128)
    sent_rows = sent.reshape(3, 2, 1024, 128)
    field_rows = field.reshape(3, 2, 1024, 128)
    back_rows = back.reshape(3, 2, 1024, 128)
    home_rows = home.reshape(3, 2, 1024, 128)
    final_rows = final.reshape(2, 2048, 128)

    def every(first_row):
        return pl.ds(first_row, 128, stride=8)

    def expand(j, carry):
        i, h = lax.div(j, 2), lax.rem(j, 2)

        @pl.when(j < 2)
        def _():
            arrived(kept.at[h], h)

        by_low = start[i, 0], start[i, 1]
        by_high = start[i, 2], start[i, 3]
        for g in range(2):
            pair = []
            for c in (2 * g, 2 * g + 1):
                below = kept_rows[h, every(2 * c), :], kept_rows[h, every(2 * c + 1), :]
                above = (
                    kept_rows[h, every(1024 + 2 * c), :],
                    kept_rows[h, every(1025 + 2 * c), :],
                )
                pair.append(add(times(below, by_low), times(above, by_high)))
            mixed = from_left(high[0], low[0], paired(*pair))
            for w in range(2):
                c = 2 * g + w
                by = turn1[i, 4 * h + c, 0], turn1[i, 4 * h + c, 1]
                re, im = times(parts(mixed, w), by)
                sent_rows[i, h, every(c), :] = re
                sent_rows[i, h, every(4 + c), :] = im
        exchange(lambda q: sent.at[i, h, q], lambda p: field.at[i, h, p], 2 + j)
        return carry

    lax.fori_loop(0, 6, expand, 0)

    scale = 1.0 / math.sqrt(MODES)
    factor = 1.0 / math.sqrt(POINTS)

    def middle(i, carry):
        for h in range(2):
            arrived(field.at[i, h], 2 + 2 * i + h)
            for g in range(2):
                pair = [
                    (field_rows[i, h, every(s), :], field_rows[i, h, every(4 + s), :])
                    for s in (2 * g, 2 * g + 1)
                ]
                mixed = from_left(high[0], low[0], paired(*pair))
                for w in range(2):
                    s = 4 * h + 2 * g + w
                    work[s, 0], work[s, 1] = parts(mixed, w)

        def rise(k, inside):
            rows = pl.ds(pl.multiple_of(8 * k, 8), 8)
            v = [
                times(
                    (work[s, 0, rows, :], work[s, 1, rows, :]),
                    (turn2[s, 0, rows, :], turn2[s, 1, rows, :]),
                )
                for s in range(8)
            ]
            v = eight(v, 1)
            for s in range(8):
                re, im = times(v[s], (turn3[s, 0, rows, :], turn3[s, 1, rows, :]))
                work[s, 0, rows, :] = re
                work[s, 1, rows, :] = im
            return inside

        lax.fori_loop(0, 16, rise, 0)

        def peak(k, inside):
            some = pl.ds(4 * k, 4)
            value = jnp.concatenate(
                [work[some, 0].reshape(512, 128), work[some, 1].reshape(512, 128)], axis=1
            )
            value = from_right(value, high[1], low[1]) * scale
            re, im = value[:, :128], value[:, 128:]
            value = jnp.concatenate(
                [(re * re - im * im) * factor, (2.0 * factor) * (re * im)], axis=1
            )
            value = from_right(value, high[0], low[0])
            re, im = times_conj(
                (value[:, :128].reshape(4, 128, 128), value[:, 128:].reshape(4, 128, 128)),
                (turn3[some, 0], turn3[some, 1]),
            )
            work[some, 0] = re
            work[some, 1] = im
            return inside

        lax.fori_loop(0, 2, peak, 0)

        def fall(k, inside):
            rows = pl.ds(pl.multiple_of(8 * k, 8), 8)
            v = eight([(work[s, 0, rows, :], work[s, 1, rows, :]) for s in range(8)], -1)
            for s in range(8):
                re, im = times_conj(v[s], (turn2[s, 0, rows, :], turn2[s, 1, rows, :]))
                work[s, 0, rows, :] = re
                work[s, 1, rows, :] = im
            return inside

        lax.fori_loop(0, 16, fall, 0)

        def part(h, inside):
            for g in range(2):
                pair = [(work[4 * h + s, 0], work[4 * h + s, 1]) for s in (2 * g, 2 * g + 1)]
                mixed = from_left(high[1], low[1], paired(*pair))
                for w in range(2):
                    s = 2 * g + w
                    re, im = parts(mixed, w)
                    back_rows[i, h, every(s), :] = re
                    back_rows[i, h, every(4 + s), :] = im
            exchange(lambda q: back.at[i, h, q], lambda p: home.at[i, h, p], 8 + 2 * i + h)
            return inside

        lax.fori_loop(0, 2, part, 0)
        return carry

    lax.fori_loop(0, 3, middle, 0)

    def gather(j, carry):
        i, h = lax.div(j, 2), lax.rem(j, 2)
        arrived(home.at[i, h], 8 + j)
        by_low = start[i, 0], start[i, 1]
        by_high = start[i, 2], start[i, 3]
        for g in range(2):
            pair = [
                times_conj(
                    (home_rows[i, h, every(c), :], home_rows[i, h, every(4 + c), :]),
                    (turn1[i, 4 * h + c, 0], turn1[i, 4 * h + c, 1]),
                )
                for c in (2 * g, 2 * g + 1)
            ]
            mixed = from_left(high[1], low[1], paired(*pair))
            for w in range(2):
                c = 2 * g + w
                value = parts(mixed, w)
                for f, by in enumerate((by_low, by_high)):
                    re, im = times_conj(value, by)
                    total[h, c, f, 0] += re
                    total[h, c, f, 1] += im

        @pl.when(i == 2)
        def _():
            for c in range(4):
                for f in range(2):
                    for r in range(2):
                        final_rows[h, every(1024 * f + 2 * c + r), :] = total[h, c, f, r]
            some = pl.ds(pl.multiple_of(8 * h, 8), 8)
            exchange(
                lambda q: final.at[h, pl.ds(2 * q, 2)],
                lambda p: out.at[:, p, some],
                14 + h,
                far_first,
            )

        return carry

    lax.fori_loop(0, 6, gather, 0)
    others = pl.ds(0, DEVICES - 1)
    double = pl.ds(0, 2 * (DEVICES - 1))
    for h in range(2):
        gone(kept.at[h, double], h)
        for i in range(3):
            gone(sent.at[i, h, others], 2 + 2 * i + h)
            gone(back.at[i, h, others], 8 + 2 * i + h)
    for h in range(2):
        arrived(final.at[h], 14 + h)
        gone(final.at[h, double], 14 + h)


def body(spectrum):
    x = spectrum.reshape(2, 2048, 128).transpose(1, 0, 2).reshape(2, 128, 16, 128)
    anywhere = pl.BlockSpec(memory_space=pl.ANY)
    held = [jnp.asarray(t) for t in tables()]
    grid = (3, 2, 128, 8, 128)
    out = pl.pallas_call(
        kernel,
        name="convolve",
        out_shape=pltpu.VMEM((2, 128, 16, 128), F32),
        in_specs=[anywhere] * (1 + len(held)),
        out_specs=anywhere,
        scratch_shapes=[
            pltpu.VMEM((2, 128, 16, 128), F32),
            *[pltpu.VMEM(t.shape, t.dtype) for t in held],
            pltpu.VMEM((2, 256, 8, 128), F32),
            pltpu.VMEM(grid, F32),
            pltpu.VMEM(grid, F32),
            pltpu.VMEM(grid, F32),
            pltpu.VMEM(grid, F32),
            pltpu.VMEM((2, 256, 8, 128), F32),
            pltpu.VMEM((2, 4, 2, 2, 128, 128), F32),
            pltpu.VMEM((8, 2, 128, 128), F32),
            pltpu.VMEM((3, 8, 2, 128, 128), F32),
            pltpu.VMEM((8, 2, 128, 128), F32),
            pltpu.VMEM((8, 2, 128, 128), F32),
            pltpu.VMEM((3, 4, 128, 128), F32),
            pltpu.SemaphoreType.DMA((8,)),
            pltpu.SemaphoreType.DMA((16,)),
            pltpu.SemaphoreType.DMA((16,)),
        ],
        compiler_params=pltpu.CompilerParams(
            collective_id=0, has_side_effects=True, vmem_limit_bytes=40 * 1024 * 1024
        ),
    )(*[pltpu.with_memory_space_constraint(t, pltpu.HBM) for t in (x, *held)])
    return out.reshape(2048, 2, 128).transpose(1, 0, 2).reshape(2, 262144)


def solution(mesh):
    return jax.shard_map(
        body,
        mesh=mesh,
        in_specs=(P(None, ("row", "col")),),
        out_specs=P(None, ("row", "col")),
        check_vma=False,
    )
```

```python
import functools
import math

import jax
import jax.numpy as jnp
import numpy as np
from jax import lax
from jax.experimental import pallas as pl
from jax.experimental.pallas import tpu as pltpu
from jax.sharding import PartitionSpec as P

B = 131072
MODES = 33554432
POINTS = 50331648
DEVICES = 128
STEP = 37


def far_to_near():
    hops = [0, 1, 2, 1]
    steps = [(STEP * k) % 128 for k in range(1, DEVICES)]
    steps = [(t // 32, t // 16 % 2, t // 4 % 4, t % 4) for t in steps]
    return sorted(steps, key=lambda t: -(hops[t[0]] + hops[t[2]] + hops[t[3]]))


FAR = far_to_near()

MESH = pl.DeviceIdType.MESH
F32 = jnp.float32
BF16 = jnp.bfloat16


def unit(turns, total):
    angle = 2.0 * np.pi * (np.asarray(turns, np.int64) % total) / total
    return np.cos(angle), np.sin(angle)


def tables():
    m = np.arange(128)
    lane = np.arange(128)
    cos, sin = unit(m[:, None] * m[None, :], 128)
    plus = np.block([[cos, -sin], [sin, cos]])
    both = np.stack([plus, plus.T]).astype(np.float32)
    high = both.astype(BF16)
    low = (both - high.astype(np.float32)).astype(BF16)
    lanes = np.zeros((3, 2, 128, 128), np.float32)
    place = np.zeros((3, 2, 128, 128), np.float32)
    columns = np.zeros((4, 128, 128), np.float32)
    for i in range(3):
        mine = i + 3 * m
        lanes[i] = unit(mine[:, None] * lane[None, :], POINTS)
        place[i] = unit(mine[:, None] * lane[None, :] * 1024, POINTS)
        re, im = unit(mine[:, None] * np.arange(8)[None, :] * 128, POINTS)
        columns[i, :, 0:8], columns[i, :, 8:16] = re, im
        columns[i, :, 16], columns[i, :, 17] = unit(i * m, 384)
        columns[i, :, 18], columns[i, :, 19] = unit(i * (m + 256), 384)
    re, im = unit(m[:, None] * np.arange(8)[None, :], 1024)
    columns[3, :, 0:8], columns[3, :, 8:16] = re, im
    inner = np.stack(unit(m[:, None] * lane[None, :], B)).astype(np.float32)
    outer = np.stack(unit(np.arange(8)[:, None] * lane[None, :], 1024)).astype(np.float32)
    return high, low, lanes, place, columns, inner, outer


def split(value):
    high = value.astype(BF16)
    return high, (value - high.astype(F32)).astype(BF16)


def from_left(high, low, value):
    left = jnp.concatenate([high, high, low], axis=1)
    top, rest = split(value)
    right = jnp.concatenate([top, rest, top], axis=0)
    return jnp.dot(left, right, preferred_element_type=F32)


def from_right(value, high, low):
    top, rest = split(value)
    left = jnp.concatenate([top, rest, top], axis=1)
    right = jnp.concatenate([high, high, low], axis=0)
    return jnp.dot(left, right, preferred_element_type=F32)


def times(a, b):
    return a[0] * b[0] - a[1] * b[1], a[0] * b[1] + a[1] * b[0]


def times_conj(a, b):
    return a[0] * b[0] + a[1] * b[1], a[1] * b[0] - a[0] * b[1]


def turn(a, sign):
    return (-a[1], a[0]) if sign > 0 else (a[1], -a[0])


def add(a, b):
    return a[0] + b[0], a[1] + b[1]


def sub(a, b):
    return a[0] - b[0], a[1] - b[1]


def four(a, b, c, d, sign):
    even, odd = add(a, c), sub(a, c)
    other, cross = add(b, d), turn(sub(b, d), sign)
    return add(even, other), add(odd, cross), sub(even, other), sub(odd, cross)


def eight(v, sign):
    even = four(v[0], v[2], v[4], v[6], sign)
    odd = four(v[1], v[3], v[5], v[7], sign)
    half = math.sqrt(0.5)
    one = turn(odd[1], sign)
    one = ((odd[1][0] + one[0]) * half, (odd[1][1] + one[1]) * half)
    two = turn(odd[2], sign)
    three = turn(odd[3], sign)
    three = ((three[0] - odd[3][0]) * half, (three[1] - odd[3][1]) * half)
    odd = (odd[0], one, two, three)
    return [add(e, o) for e, o in zip(even, odd)] + [sub(e, o) for e, o in zip(even, odd)]


def paired(first, second):
    re = jnp.concatenate([first[0], second[0]], axis=1)
    im = jnp.concatenate([first[1], second[1]], axis=1)
    return jnp.concatenate([re, im], axis=0)


def parts(value, which):
    cols = slice(128 * which, 128 * which + 128)
    return value[:128, cols], value[128:, cols]


def wrap(value, size):
    return jnp.where(value >= size, value - size, value)


def kernel(
    x_far,
    high_far,
    low_far,
    lanes_far,
    place_far,
    columns_far,
    inner_far,
    outer_far,
    out,
    x,
    high,
    low,
    lanes,
    place,
    columns,
    inner,
    outer,
    kept,
    sent,
    field,
    back,
    home,
    final,
    total,
    work,
    turn1,
    turn2,
    turn3,
    start,
    load,
    send,
    recv,
):
    row = lax.axis_index("row")
    col = lax.axis_index("col")
    me = row * 16 + col

    loads = [
        pltpu.make_async_copy(far, near, load.at[k])
        for k, (far, near) in enumerate(
            (
                (x_far, x),
                (high_far, high),
                (low_far, low),
                (lanes_far, lanes),
                (place_far, place),
                (columns_far, columns),
                (inner_far, inner),
                (outer_far, outer),
            )
        )
    ]
    for one in loads:
        one.start()

    cols = [wrap(col + c, 16) for c in range(16)]

    def each_peer(act):
        def group(o, base):
            rows = [wrap(base + k, 8) for k in range(8)]
            for u in range(16):
                to_row, to_col = rows[(STEP * u // 16) % 8], cols[STEP * u % 16]
                if u == 0:
                    pl.when(o > 0)(functools.partial(act, to_row, to_col))
                else:
                    act(to_row, to_col)
            return wrap(base + STEP % 8, 8)

        lax.fori_loop(0, 8, group, row)

    at_x, at_core = lax.div(row, 2), lax.rem(row, 2)
    at_z, at_y = lax.div(col, 4), lax.rem(col, 4)
    to_x = [wrap(at_x + d, 4) * 2 for d in range(4)]
    to_core = [wrap(at_core + d, 2) for d in range(2)]
    to_z = [wrap(at_z + d, 4) * 4 for d in range(4)]
    to_y = [wrap(at_y + d, 4) for d in range(4)]

    def far_first(act):
        for dx, dc, dz, dy in FAR:
            act(to_x[dx] + to_core[dc], to_z[dz] + to_y[dy])

    barrier = pltpu.get_barrier_semaphore()

    def greet(to_row, to_col):
        pl.semaphore_signal(barrier, inc=1, device_id=(to_row, to_col), device_id_type=MESH)

    far_first(greet)
    loads[0].wait()
    pl.semaphore_wait(barrier, DEVICES - 1)

    def exchange(src_of, dst_of, phase, order=each_peer):
        mine = dst_of(me)

        def one(to_row, to_col):
            pltpu.make_async_remote_copy(
                src_ref=src_of(to_row * 16 + to_col),
                dst_ref=mine,
                send_sem=send.at[phase],
                recv_sem=recv.at[phase],
                device_id=(to_row, to_col),
                device_id_type=MESH,
            ).start()

        order(one)
        pltpu.make_async_copy(src_of(me), mine, recv.at[phase]).start()

    def arrived(ref, phase):
        pltpu.make_async_copy(ref, ref, recv.at[phase]).wait()

    def gone(ref, phase):
        pltpu.make_async_copy(ref, ref, send.at[phase]).wait()

    def first(h, carry):
        some = pl.ds(pl.multiple_of(8 * h, 8), 8)
        exchange(lambda q: x.at[:, q, some], lambda p: kept.at[h, pl.ds(2 * p, 2)], h)
        return carry

    lax.fori_loop(0, 2, first, 0)
    for one in loads[1:]:
        one.wait()

    here = lax.broadcasted_iota(jnp.int32, (128, 128), 1) == me

    def prepare(i, carry):
        own = [
            jnp.sum(jnp.where(here, place[i, r], 0.0), axis=1, keepdims=True) for r in range(2)
        ]
        base = lanes[i, 0], lanes[i, 1]
        for c in range(8):
            step = columns[i, :, c : c + 1], columns[i, :, 8 + c : 9 + c]
            re, im = times(times(own, step), base)
            turn1[i, c, 0], turn1[i, c, 1] = re, im
        for k in range(4):
            start[i, k] = jnp.broadcast_to(columns[i, :, 16 + k : 17 + k], (128, 128))
        return carry

    lax.fori_loop(0, 3, prepare, 0)
    for s in range(8):
        for r in range(2):
            turn2[s, r] = jnp.broadcast_to(columns[3, :, 8 * r + s : 8 * r + s + 1], (128, 128))
        re, im = times((inner[0], inner[1]), (outer[0, s : s + 1], outer[1, s : s + 1]))
        turn3[s, 0], turn3[s, 1] = re, im
    total[...] = jnp.zeros_like(total)

    kept_rows = kept.reshape(2, 2048, 128)
    sent_rows = sent.reshape(3, 2, 1024, 128)
    field_rows = field.reshape(3, 2, 1024, 128)
    back_rows = back.reshape(3, 2, 1024, 128)
    home_rows = home.reshape(3, 2, 1024, 128)
    final_rows = final.reshape(2, 2048, 128)

    def every(first_row):
        return pl.ds(first_row, 128, stride=8)

    def expand(j, carry):
        i = jnp.where(j < 4, lax.rem(j, 2), 2)
        h = jnp.where(j < 4, lax.div(j, 2), j - 4)

        @pl.when((j < 4) & (i == 0))
        def _():
            arrived(kept.at[h], h)

        by_low = start[i, 0], start[i, 1]
        by_high = start[i, 2], start[i, 3]
        for g in range(2):
            pair = []
            for c in (2 * g, 2 * g + 1):
                below = kept_rows[h, every(2 * c), :], kept_rows[h, every(2 * c + 1), :]
                above = (
                    kept_rows[h, every(1024 + 2 * c), :],
                    kept_rows[h, every(1025 + 2 * c), :],
                )
                pair.append(add(times(below, by_low), times(above, by_high)))
            mixed = from_left(high[0], low[0], paired(*pair))
            for w in range(2):
                c = 2 * g + w
                by = turn1[i, 4 * h + c, 0], turn1[i, 4 * h + c, 1]
                re, im = times(parts(mixed, w), by)
                sent_rows[i, h, every(c), :] = re
                sent_rows[i, h, every(4 + c), :] = im
        exchange(lambda q: sent.at[i, h, q], lambda p: field.at[i, h, p], 2 + 2 * i + h)
        return carry

    lax.fori_loop(0, 6, expand, 0)

    scale = 1.0 / math.sqrt(MODES)
    factor = 1.0 / math.sqrt(POINTS)

    def middle(i, carry):
        for h in range(2):
            arrived(field.at[i, h], 2 + 2 * i + h)
            for g in range(2):
                pair = [
                    (field_rows[i, h, every(s), :], field_rows[i, h, every(4 + s), :])
                    for s in (2 * g, 2 * g + 1)
                ]
                mixed = from_left(high[0], low[0], paired(*pair))
                for w in range(2):
                    s = 4 * h + 2 * g + w
                    work[s, 0], work[s, 1] = parts(mixed, w)

        def rise(k, inside):
            rows = pl.ds(pl.multiple_of(8 * k, 8), 8)
            v = [
                times(
                    (work[s, 0, rows, :], work[s, 1, rows, :]),
                    (turn2[s, 0, rows, :], turn2[s, 1, rows, :]),
                )
                for s in range(8)
            ]
            v = eight(v, 1)
            for s in range(8):
                re, im = times(v[s], (turn3[s, 0, rows, :], turn3[s, 1, rows, :]))
                work[s, 0, rows, :] = re
                work[s, 1, rows, :] = im
            return inside

        lax.fori_loop(0, 16, rise, 0)

        def peak(k, inside):
            some = pl.ds(4 * k, 4)
            value = jnp.concatenate(
                [work[some, 0].reshape(512, 128), work[some, 1].reshape(512, 128)], axis=1
            )
            value = from_right(value, high[1], low[1]) * scale
            re, im = value[:, :128], value[:, 128:]
            value = jnp.concatenate(
                [(re * re - im * im) * factor, (2.0 * factor) * (re * im)], axis=1
            )
            value = from_right(value, high[0], low[0])
            re, im = times_conj(
                (value[:, :128].reshape(4, 128, 128), value[:, 128:].reshape(4, 128, 128)),
                (turn3[some, 0], turn3[some, 1]),
            )
            work[some, 0] = re
            work[some, 1] = im
            return inside

        lax.fori_loop(0, 2, peak, 0)

        def fall(k, inside):
            rows = pl.ds(pl.multiple_of(8 * k, 8), 8)
            v = eight([(work[s, 0, rows, :], work[s, 1, rows, :]) for s in range(8)], -1)
            for s in range(8):
                re, im = times_conj(v[s], (turn2[s, 0, rows, :], turn2[s, 1, rows, :]))
                work[s, 0, rows, :] = re
                work[s, 1, rows, :] = im
            return inside

        lax.fori_loop(0, 16, fall, 0)

        def part(h, inside):
            for g in range(2):
                pair = [(work[4 * h + s, 0], work[4 * h + s, 1]) for s in (2 * g, 2 * g + 1)]
                mixed = from_left(high[1], low[1], paired(*pair))
                for w in range(2):
                    s = 2 * g + w
                    re, im = parts(mixed, w)
                    back_rows[i, h, every(s), :] = re
                    back_rows[i, h, every(4 + s), :] = im

            def give(k, within):
                exchange(
                    lambda q: back.at[k, h, q], lambda p: home.at[k, h, p], 8 + 2 * k + h
                )
                return within

            first_one = jnp.where(h == 0, i, 0)
            past_last = jnp.where(h == 0, i + 1, jnp.where(i == 2, 3, 0))
            lax.fori_loop(first_one, past_last, give, 0)
            return inside

        lax.fori_loop(0, 2, part, 0)
        return carry

    lax.fori_loop(0, 3, middle, 0)

    def gather(j, carry):
        i, h = lax.rem(j, 3), lax.div(j, 3)
        arrived(home.at[i, h], 8 + 2 * i + h)
        by_low = start[i, 0], start[i, 1]
        by_high = start[i, 2], start[i, 3]
        for g in range(2):
            pair = [
                times_conj(
                    (home_rows[i, h, every(c), :], home_rows[i, h, every(4 + c), :]),
                    (turn1[i, 4 * h + c, 0], turn1[i, 4 * h + c, 1]),
                )
                for c in (2 * g, 2 * g + 1)
            ]
            mixed = from_left(high[1], low[1], paired(*pair))
            for w in range(2):
                c = 2 * g + w
                value = parts(mixed, w)
                for f, by in enumerate((by_low, by_high)):
                    re, im = times_conj(value, by)
                    total[h, c, f, 0] += re
                    total[h, c, f, 1] += im

        @pl.when(i == 2)
        def _():
            for c in range(4):
                for f in range(2):
                    for r in range(2):
                        final_rows[h, every(1024 * f + 2 * c + r), :] = total[h, c, f, r]
            some = pl.ds(pl.multiple_of(8 * h, 8), 8)
            exchange(
                lambda q: final.at[h, pl.ds(2 * q, 2)],
                lambda p: out.at[:, p, some],
                14 + h,
                far_first,
            )

        return carry

    lax.fori_loop(0, 6, gather, 0)
    others = pl.ds(0, DEVICES - 1)
    double = pl.ds(0, 2 * (DEVICES - 1))
    for h in range(2):
        gone(kept.at[h, double], h)
        for i in range(3):
            gone(sent.at[i, h, others], 2 + 2 * i + h)
            gone(back.at[i, h, others], 8 + 2 * i + h)
    for h in range(2):
        arrived(final.at[h], 14 + h)
        gone(final.at[h, double], 14 + h)


def body(spectrum):
    x = spectrum.reshape(2, 2048, 128).transpose(1, 0, 2).reshape(2, 128, 16, 128)
    anywhere = pl.BlockSpec(memory_space=pl.ANY)
    held = [jnp.asarray(t) for t in tables()]
    grid = (3, 2, 128, 8, 128)
    out = pl.pallas_call(
        kernel,
        name="convolve",
        out_shape=pltpu.VMEM((2, 128, 16, 128), F32),
        in_specs=[anywhere] * (1 + len(held)),
        out_specs=anywhere,
        scratch_shapes=[
            pltpu.VMEM((2, 128, 16, 128), F32),
            *[pltpu.VMEM(t.shape, t.dtype) for t in held],
            pltpu.VMEM((2, 256, 8, 128), F32),
            pltpu.VMEM(grid, F32),
            pltpu.VMEM(grid, F32),
            pltpu.VMEM(grid, F32),
            pltpu.VMEM(grid, F32),
            pltpu.VMEM((2, 256, 8, 128), F32),
            pltpu.VMEM((2, 4, 2, 2, 128, 128), F32),
            pltpu.VMEM((8, 2, 128, 128), F32),
            pltpu.VMEM((3, 8, 2, 128, 128), F32),
            pltpu.VMEM((8, 2, 128, 128), F32),
            pltpu.VMEM((8, 2, 128, 128), F32),
            pltpu.VMEM((3, 4, 128, 128), F32),
            pltpu.SemaphoreType.DMA((8,)),
            pltpu.SemaphoreType.DMA((16,)),
            pltpu.SemaphoreType.DMA((16,)),
        ],
        compiler_params=pltpu.CompilerParams(
            collective_id=0, has_side_effects=True, vmem_limit_bytes=40 * 1024 * 1024
        ),
    )(*[pltpu.with_memory_space_constraint(t, pltpu.HBM) for t in (x, *held)])
    return out.reshape(2048, 2, 128).transpose(1, 0, 2).reshape(2, 262144)


def solution(mesh):
    return jax.shard_map(
        body,
        mesh=mesh,
        in_specs=(P(None, ("row", "col")),),
        out_specs=P(None, ("row", "col")),
        check_vma=False,
    )
```

```python
import functools
import math

import jax
import jax.numpy as jnp
import numpy as np
from jax import lax
from jax.experimental import pallas as pl
from jax.experimental.pallas import tpu as pltpu
from jax.sharding import PartitionSpec as P

B = 131072
MODES = 33554432
POINTS = 50331648
DEVICES = 128
STEP = 37


def far_to_near():
    hops = [0, 1, 2, 1]
    steps = [(STEP * k) % 128 for k in range(1, DEVICES)]
    steps = [(t // 32, t // 16 % 2, t // 4 % 4, t % 4) for t in steps]
    return sorted(steps, key=lambda t: -(hops[t[0]] + hops[t[2]] + hops[t[3]]))


FAR = far_to_near()


def paired_steps():
    order = []
    for k in range(1, DEVICES):
        t = (STEP * k) % 128
        step = (t // 32, t // 16 % 2, t // 4 % 4, t % 4)
        other = (-step[0] % 4, step[1], -step[2] % 4, -step[3] % 4)
        for one in (step, other):
            if one not in order:
                order.append(one)
    return order


MIX = paired_steps()

MESH = pl.DeviceIdType.MESH
F32 = jnp.float32
BF16 = jnp.bfloat16


def unit(turns, total):
    angle = 2.0 * np.pi * (np.asarray(turns, np.int64) % total) / total
    return np.cos(angle), np.sin(angle)


def tables():
    m = np.arange(128)
    lane = np.arange(128)
    cos, sin = unit(m[:, None] * m[None, :], 128)
    plus = np.block([[cos, -sin], [sin, cos]])
    both = np.stack([plus, plus.T]).astype(np.float32)
    high = both.astype(BF16)
    low = (both - high.astype(np.float32)).astype(BF16)
    lanes = np.zeros((3, 2, 128, 128), np.float32)
    place = np.zeros((3, 2, 128, 128), np.float32)
    columns = np.zeros((4, 128, 128), np.float32)
    for i in range(3):
        mine = i + 3 * m
        lanes[i] = unit(mine[:, None] * lane[None, :], POINTS)
        place[i] = unit(mine[:, None] * lane[None, :] * 1024, POINTS)
        re, im = unit(mine[:, None] * np.arange(8)[None, :] * 128, POINTS)
        columns[i, :, 0:8], columns[i, :, 8:16] = re, im
        columns[i, :, 16], columns[i, :, 17] = unit(i * m, 384)
        columns[i, :, 18], columns[i, :, 19] = unit(i * (m + 256), 384)
    re, im = unit(m[:, None] * np.arange(8)[None, :], 1024)
    columns[3, :, 0:8], columns[3, :, 8:16] = re, im
    inner = np.stack(unit(m[:, None] * lane[None, :], B)).astype(np.float32)
    outer = np.stack(unit(np.arange(8)[:, None] * lane[None, :], 1024)).astype(np.float32)
    return high, low, lanes, place, columns, inner, outer


def split(value):
    high = value.astype(BF16)
    return high, (value - high.astype(F32)).astype(BF16)


def from_left(high, low, value):
    left = jnp.concatenate([high, high, low], axis=1)
    top, rest = split(value)
    right = jnp.concatenate([top, rest, top], axis=0)
    return jnp.dot(left, right, preferred_element_type=F32)


def from_right(value, high, low):
    top, rest = split(value)
    left = jnp.concatenate([top, rest, top], axis=1)
    right = jnp.concatenate([high, high, low], axis=0)
    return jnp.dot(left, right, preferred_element_type=F32)


def times(a, b):
    return a[0] * b[0] - a[1] * b[1], a[0] * b[1] + a[1] * b[0]


def times_conj(a, b):
    return a[0] * b[0] + a[1] * b[1], a[1] * b[0] - a[0] * b[1]


def turn(a, sign):
    return (-a[1], a[0]) if sign > 0 else (a[1], -a[0])


def add(a, b):
    return a[0] + b[0], a[1] + b[1]


def sub(a, b):
    return a[0] - b[0], a[1] - b[1]


def four(a, b, c, d, sign):
    even, odd = add(a, c), sub(a, c)
    other, cross = add(b, d), turn(sub(b, d), sign)
    return add(even, other), add(odd, cross), sub(even, other), sub(odd, cross)


def eight(v, sign):
    even = four(v[0], v[2], v[4], v[6], sign)
    odd = four(v[1], v[3], v[5], v[7], sign)
    half = math.sqrt(0.5)
    one = turn(odd[1], sign)
    one = ((odd[1][0] + one[0]) * half, (odd[1][1] + one[1]) * half)
    two = turn(odd[2], sign)
    three = turn(odd[3], sign)
    three = ((three[0] - odd[3][0]) * half, (three[1] - odd[3][1]) * half)
    odd = (odd[0], one, two, three)
    return [add(e, o) for e, o in zip(even, odd)] + [sub(e, o) for e, o in zip(even, odd)]


def paired(first, second):
    re = jnp.concatenate([first[0], second[0]], axis=1)
    im = jnp.concatenate([first[1], second[1]], axis=1)
    return jnp.concatenate([re, im], axis=0)


def parts(value, which):
    cols = slice(128 * which, 128 * which + 128)
    return value[:128, cols], value[128:, cols]


def wrap(value, size):
    return jnp.where(value >= size, value - size, value)


def kernel(
    x_far,
    high_far,
    low_far,
    lanes_far,
    place_far,
    columns_far,
    inner_far,
    outer_far,
    out,
    x,
    high,
    low,
    lanes,
    place,
    columns,
    inner,
    outer,
    kept,
    sent,
    field,
    back,
    home,
    final,
    total,
    work,
    turn1,
    turn2,
    turn3,
    start,
    load,
    send,
    recv,
):
    row = lax.axis_index("row")
    col = lax.axis_index("col")
    me = row * 16 + col

    loads = [
        pltpu.make_async_copy(far, near, load.at[k])
        for k, (far, near) in enumerate(
            (
                (x_far, x),
                (high_far, high),
                (low_far, low),
                (lanes_far, lanes),
                (place_far, place),
                (columns_far, columns),
                (inner_far, inner),
                (outer_far, outer),
            )
        )
    ]
    for one in loads:
        one.start()

    cols = [wrap(col + c, 16) for c in range(16)]

    def each_peer(act):
        def group(o, base):
            rows = [wrap(base + k, 8) for k in range(8)]
            for u in range(16):
                to_row, to_col = rows[(STEP * u // 16) % 8], cols[STEP * u % 16]
                if u == 0:
                    pl.when(o > 0)(functools.partial(act, to_row, to_col))
                else:
                    act(to_row, to_col)
            return wrap(base + STEP % 8, 8)

        lax.fori_loop(0, 8, group, row)

    at_x, at_core = lax.div(row, 2), lax.rem(row, 2)
    at_z, at_y = lax.div(col, 4), lax.rem(col, 4)
    to_x = [wrap(at_x + d, 4) * 2 for d in range(4)]
    to_core = [wrap(at_core + d, 2) for d in range(2)]
    to_z = [wrap(at_z + d, 4) * 4 for d in range(4)]
    to_y = [wrap(at_y + d, 4) for d in range(4)]

    def far_first(act):
        for dx, dc, dz, dy in FAR:
            act(to_x[dx] + to_core[dc], to_z[dz] + to_y[dy])

    def by_mix(act):
        for dx, dc, dz, dy in MIX:
            act(to_x[dx] + to_core[dc], to_z[dz] + to_y[dy])

    barrier = pltpu.get_barrier_semaphore()

    def greet(to_row, to_col):
        pl.semaphore_signal(barrier, inc=1, device_id=(to_row, to_col), device_id_type=MESH)

    far_first(greet)
    loads[0].wait()
    pl.semaphore_wait(barrier, DEVICES - 1)

    def exchange(src_of, dst_of, phase, order=by_mix):
        mine = dst_of(me)

        def one(to_row, to_col):
            pltpu.make_async_remote_copy(
                src_ref=src_of(to_row * 16 + to_col),
                dst_ref=mine,
                send_sem=send.at[phase],
                recv_sem=recv.at[phase],
                device_id=(to_row, to_col),
                device_id_type=MESH,
            ).start()

        order(one)
        pltpu.make_async_copy(src_of(me), mine, recv.at[phase]).start()

    def arrived(ref, phase):
        pltpu.make_async_copy(ref, ref, recv.at[phase]).wait()

    def gone(ref, phase):
        pltpu.make_async_copy(ref, ref, send.at[phase]).wait()

    def first(h, carry):
        some = pl.ds(pl.multiple_of(8 * h, 8), 8)
        exchange(lambda q: x.at[:, q, some], lambda p: kept.at[h, pl.ds(2 * p, 2)], h)
        return carry

    lax.fori_loop(0, 2, first, 0)
    for one in loads[1:]:
        one.wait()

    here = lax.broadcasted_iota(jnp.int32, (128, 128), 1) == me

    def prepare(i, carry):
        own = [
            jnp.sum(jnp.where(here, place[i, r], 0.0), axis=1, keepdims=True) for r in range(2)
        ]
        base = lanes[i, 0], lanes[i, 1]
        for c in range(8):
            step = columns[i, :, c : c + 1], columns[i, :, 8 + c : 9 + c]
            re, im = times(times(own, step), base)
            turn1[i, c, 0], turn1[i, c, 1] = re, im
        for k in range(4):
            start[i, k] = jnp.broadcast_to(columns[i, :, 16 + k : 17 + k], (128, 128))
        return carry

    lax.fori_loop(0, 3, prepare, 0)
    for s in range(8):
        for r in range(2):
            turn2[s, r] = jnp.broadcast_to(columns[3, :, 8 * r + s : 8 * r + s + 1], (128, 128))
        re, im = times((inner[0], inner[1]), (outer[0, s : s + 1], outer[1, s : s + 1]))
        turn3[s, 0], turn3[s, 1] = re, im
    total[...] = jnp.zeros_like(total)

    kept_rows = kept.reshape(2, 2048, 128)
    sent_rows = sent.reshape(3, 2, 1024, 128)
    field_rows = field.reshape(3, 2, 1024, 128)
    back_rows = back.reshape(3, 2, 1024, 128)
    home_rows = home.reshape(3, 2, 1024, 128)
    final_rows = final.reshape(2, 2048, 128)

    def every(first_row):
        return pl.ds(first_row, 128, stride=8)

    def expand(j, carry):
        i = jnp.where(j < 4, lax.rem(j, 2), 2)
        h = jnp.where(j < 4, lax.div(j, 2), j - 4)

        @pl.when((j < 4) & (i == 0))
        def _():
            arrived(kept.at[h], h)

        by_low = start[i, 0], start[i, 1]
        by_high = start[i, 2], start[i, 3]
        for g in range(2):
            pair = []
            for c in (2 * g, 2 * g + 1):
                below = kept_rows[h, every(2 * c), :], kept_rows[h, every(2 * c + 1), :]
                above = (
                    kept_rows[h, every(1024 + 2 * c), :],
                    kept_rows[h, every(1025 + 2 * c), :],
                )
                pair.append(add(times(below, by_low), times(above, by_high)))
            mixed = from_left(high[0], low[0], paired(*pair))
            for w in range(2):
                c = 2 * g + w
                by = turn1[i, 4 * h + c, 0], turn1[i, 4 * h + c, 1]
                re, im = times(parts(mixed, w), by)
                sent_rows[i, h, every(c), :] = re
                sent_rows[i, h, every(4 + c), :] = im
        exchange(lambda q: sent.at[i, h, q], lambda p: field.at[i, h, p], 2 + 2 * i + h)
        return carry

    lax.fori_loop(0, 6, expand, 0)

    scale = 1.0 / math.sqrt(MODES)
    factor = 1.0 / math.sqrt(POINTS)

    def middle(i, carry):
        for h in range(2):
            arrived(field.at[i, h], 2 + 2 * i + h)
            for g in range(2):
                pair = [
                    (field_rows[i, h, every(s), :], field_rows[i, h, every(4 + s), :])
                    for s in (2 * g, 2 * g + 1)
                ]
                mixed = from_left(high[0], low[0], paired(*pair))
                for w in range(2):
                    s = 4 * h + 2 * g + w
                    work[s, 0], work[s, 1] = parts(mixed, w)

        def rise(k, inside):
            rows = pl.ds(pl.multiple_of(8 * k, 8), 8)
            v = [
                times(
                    (work[s, 0, rows, :], work[s, 1, rows, :]),
                    (turn2[s, 0, rows, :], turn2[s, 1, rows, :]),
                )
                for s in range(8)
            ]
            v = eight(v, 1)
            for s in range(8):
                re, im = times(v[s], (turn3[s, 0, rows, :], turn3[s, 1, rows, :]))
                work[s, 0, rows, :] = re
                work[s, 1, rows, :] = im
            return inside

        lax.fori_loop(0, 16, rise, 0)

        def peak(k, inside):
            some = pl.ds(4 * k, 4)
            value = jnp.concatenate(
                [work[some, 0].reshape(512, 128), work[some, 1].reshape(512, 128)], axis=1
            )
            value = from_right(value, high[1], low[1]) * scale
            re, im = value[:, :128], value[:, 128:]
            value = jnp.concatenate(
                [(re * re - im * im) * factor, (2.0 * factor) * (re * im)], axis=1
            )
            value = from_right(value, high[0], low[0])
            re, im = times_conj(
                (value[:, :128].reshape(4, 128, 128), value[:, 128:].reshape(4, 128, 128)),
                (turn3[some, 0], turn3[some, 1]),
            )
            work[some, 0] = re
            work[some, 1] = im
            return inside

        lax.fori_loop(0, 2, peak, 0)

        def fall(k, inside):
            rows = pl.ds(pl.multiple_of(8 * k, 8), 8)
            v = eight([(work[s, 0, rows, :], work[s, 1, rows, :]) for s in range(8)], -1)
            for s in range(8):
                re, im = times_conj(v[s], (turn2[s, 0, rows, :], turn2[s, 1, rows, :]))
                work[s, 0, rows, :] = re
                work[s, 1, rows, :] = im
            return inside

        lax.fori_loop(0, 16, fall, 0)

        def part(h, inside):
            for g in range(2):
                pair = [(work[4 * h + s, 0], work[4 * h + s, 1]) for s in (2 * g, 2 * g + 1)]
                mixed = from_left(high[1], low[1], paired(*pair))
                for w in range(2):
                    s = 2 * g + w
                    re, im = parts(mixed, w)
                    back_rows[i, h, every(s), :] = re
                    back_rows[i, h, every(4 + s), :] = im

            def give(k, within):
                exchange(
                    lambda q: back.at[k, h, q], lambda p: home.at[k, h, p], 8 + 2 * k + h
                )
                return within

            first_one = jnp.where(h == 0, i, 0)
            past_last = jnp.where(h == 0, i + 1, jnp.where(i == 2, 3, 0))
            lax.fori_loop(first_one, past_last, give, 0)
            return inside

        lax.fori_loop(0, 2, part, 0)
        return carry

    lax.fori_loop(0, 3, middle, 0)

    def gather(j, carry):
        i, h = lax.rem(j, 3), lax.div(j, 3)
        arrived(home.at[i, h], 8 + 2 * i + h)
        by_low = start[i, 0], start[i, 1]
        by_high = start[i, 2], start[i, 3]
        for g in range(2):
            pair = [
                times_conj(
                    (home_rows[i, h, every(c), :], home_rows[i, h, every(4 + c), :]),
                    (turn1[i, 4 * h + c, 0], turn1[i, 4 * h + c, 1]),
                )
                for c in (2 * g, 2 * g + 1)
            ]
            mixed = from_left(high[1], low[1], paired(*pair))
            for w in range(2):
                c = 2 * g + w
                value = parts(mixed, w)
                for f, by in enumerate((by_low, by_high)):
                    re, im = times_conj(value, by)
                    total[h, c, f, 0] += re
                    total[h, c, f, 1] += im

        @pl.when(i == 2)
        def _():
            for c in range(4):
                for f in range(2):
                    for r in range(2):
                        final_rows[h, every(1024 * f + 2 * c + r), :] = total[h, c, f, r]
            some = pl.ds(pl.multiple_of(8 * h, 8), 8)
            exchange(
                lambda q: final.at[h, pl.ds(2 * q, 2)],
                lambda p: out.at[:, p, some],
                14 + h,
                far_first,
            )

        return carry

    lax.fori_loop(0, 6, gather, 0)
    others = pl.ds(0, DEVICES - 1)
    double = pl.ds(0, 2 * (DEVICES - 1))
    for h in range(2):
        gone(kept.at[h, double], h)
        for i in range(3):
            gone(sent.at[i, h, others], 2 + 2 * i + h)
            gone(back.at[i, h, others], 8 + 2 * i + h)
    for h in range(2):
        arrived(final.at[h], 14 + h)
        gone(final.at[h, double], 14 + h)


def body(spectrum):
    x = spectrum.reshape(2, 2048, 128).transpose(1, 0, 2).reshape(2, 128, 16, 128)
    anywhere = pl.BlockSpec(memory_space=pl.ANY)
    held = [jnp.asarray(t) for t in tables()]
    grid = (3, 2, 128, 8, 128)
    out = pl.pallas_call(
        kernel,
        name="convolve",
        out_shape=pltpu.VMEM((2, 128, 16, 128), F32),
        in_specs=[anywhere] * (1 + len(held)),
        out_specs=anywhere,
        scratch_shapes=[
            pltpu.VMEM((2, 128, 16, 128), F32),
            *[pltpu.VMEM(t.shape, t.dtype) for t in held],
            pltpu.VMEM((2, 256, 8, 128), F32),
            pltpu.VMEM(grid, F32),
            pltpu.VMEM(grid, F32),
            pltpu.VMEM(grid, F32),
            pltpu.VMEM(grid, F32),
            pltpu.VMEM((2, 256, 8, 128), F32),
            pltpu.VMEM((2, 4, 2, 2, 128, 128), F32),
            pltpu.VMEM((8, 2, 128, 128), F32),
            pltpu.VMEM((3, 8, 2, 128, 128), F32),
            pltpu.VMEM((8, 2, 128, 128), F32),
            pltpu.VMEM((8, 2, 128, 128), F32),
            pltpu.VMEM((3, 4, 128, 128), F32),
            pltpu.SemaphoreType.DMA((8,)),
            pltpu.SemaphoreType.DMA((16,)),
            pltpu.SemaphoreType.DMA((16,)),
        ],
        compiler_params=pltpu.CompilerParams(
            collective_id=0, has_side_effects=True, vmem_limit_bytes=40 * 1024 * 1024
        ),
    )(*[pltpu.with_memory_space_constraint(t, pltpu.HBM) for t in (x, *held)])
    return out.reshape(2048, 2, 128).transpose(1, 0, 2).reshape(2, 262144)


def solution(mesh):
    return jax.shard_map(
        body,
        mesh=mesh,
        in_specs=(P(None, ("row", "col")),),
        out_specs=P(None, ("row", "col")),
        check_vma=False,
    )
```

```python
import functools
import math

import jax
import jax.numpy as jnp
import numpy as np
from jax import lax
from jax.experimental import pallas as pl
from jax.experimental.pallas import tpu as pltpu
from jax.sharding import PartitionSpec as P

B = 131072
MODES = 33554432
POINTS = 50331648
DEVICES = 128
STEP = 37


def far_to_near():
    hops = [0, 1, 2, 1]
    steps = [(STEP * k) % 128 for k in range(1, DEVICES)]
    steps = [(t // 32, t // 16 % 2, t // 4 % 4, t % 4) for t in steps]
    return sorted(steps, key=lambda t: -(hops[t[0]] + hops[t[2]] + hops[t[3]]))


FAR = far_to_near()

MESH = pl.DeviceIdType.MESH
F32 = jnp.float32
BF16 = jnp.bfloat16


def unit(turns, total):
    angle = 2.0 * np.pi * (np.asarray(turns, np.int64) % total) / total
    return np.cos(angle), np.sin(angle)


def tables():
    m = np.arange(128)
    lane = np.arange(128)
    cos, sin = unit(m[:, None] * m[None, :], 128)
    plus = np.block([[cos, -sin], [sin, cos]])
    both = np.stack([plus, plus.T]).astype(np.float32)
    high = both.astype(BF16)
    low = (both - high.astype(np.float32)).astype(BF16)
    lanes = np.zeros((3, 2, 128, 128), np.float32)
    place = np.zeros((3, 2, 128, 128), np.float32)
    columns = np.zeros((4, 128, 128), np.float32)
    for i in range(3):
        mine = i + 3 * m
        lanes[i] = unit(mine[:, None] * lane[None, :], POINTS)
        place[i] = unit(mine[:, None] * lane[None, :] * 1024, POINTS)
        re, im = unit(mine[:, None] * np.arange(8)[None, :] * 128, POINTS)
        columns[i, :, 0:8], columns[i, :, 8:16] = re, im
        columns[i, :, 16], columns[i, :, 17] = unit(i * m, 384)
        columns[i, :, 18], columns[i, :, 19] = unit(i * (m + 256), 384)
    re, im = unit(m[:, None] * np.arange(8)[None, :], 1024)
    columns[3, :, 0:8], columns[3, :, 8:16] = re, im
    inner = np.stack(unit(m[:, None] * lane[None, :], B)).astype(np.float32)
    outer = np.stack(unit(np.arange(8)[:, None] * lane[None, :], 1024)).astype(np.float32)
    return high, low, lanes, place, columns, inner, outer


def split(value):
    high = value.astype(BF16)
    return high, (value - high.astype(F32)).astype(BF16)


def from_left(high, low, value):
    left = jnp.concatenate([high, high, low], axis=1)
    top, rest = split(value)
    right = jnp.concatenate([top, rest, top], axis=0)
    return jnp.dot(left, right, preferred_element_type=F32)


def from_right(value, high, low):
    top, rest = split(value)
    left = jnp.concatenate([top, rest, top], axis=1)
    right = jnp.concatenate([high, high, low], axis=0)
    return jnp.dot(left, right, preferred_element_type=F32)


def times(a, b):
    return a[0] * b[0] - a[1] * b[1], a[0] * b[1] + a[1] * b[0]


def times_conj(a, b):
    return a[0] * b[0] + a[1] * b[1], a[1] * b[0] - a[0] * b[1]


def turn(a, sign):
    return (-a[1], a[0]) if sign > 0 else (a[1], -a[0])


def add(a, b):
    return a[0] + b[0], a[1] + b[1]


def sub(a, b):
    return a[0] - b[0], a[1] - b[1]


def four(a, b, c, d, sign):
    even, odd = add(a, c), sub(a, c)
    other, cross = add(b, d), turn(sub(b, d), sign)
    return add(even, other), add(odd, cross), sub(even, other), sub(odd, cross)


def eight(v, sign):
    even = four(v[0], v[2], v[4], v[6], sign)
    odd = four(v[1], v[3], v[5], v[7], sign)
    half = math.sqrt(0.5)
    one = turn(odd[1], sign)
    one = ((odd[1][0] + one[0]) * half, (odd[1][1] + one[1]) * half)
    two = turn(odd[2], sign)
    three = turn(odd[3], sign)
    three = ((three[0] - odd[3][0]) * half, (three[1] - odd[3][1]) * half)
    odd = (odd[0], one, two, three)
    return [add(e, o) for e, o in zip(even, odd)] + [sub(e, o) for e, o in zip(even, odd)]


def paired(first, second):
    re = jnp.concatenate([first[0], second[0]], axis=1)
    im = jnp.concatenate([first[1], second[1]], axis=1)
    return jnp.concatenate([re, im], axis=0)


def parts(value, which):
    cols = slice(128 * which, 128 * which + 128)
    return value[:128, cols], value[128:, cols]


def wrap(value, size):
    return jnp.where(value >= size, value - size, value)


def kernel(
    x_far,
    high_far,
    low_far,
    lanes_far,
    place_far,
    columns_far,
    inner_far,
    outer_far,
    out,
    x,
    high,
    low,
    lanes,
    place,
    columns,
    inner,
    outer,
    kept,
    sent,
    field,
    back,
    home,
    final,
    total,
    work,
    turn1,
    turn2,
    turn3,
    start,
    load,
    send,
    recv,
):
    row = lax.axis_index("row")
    col = lax.axis_index("col")
    me = row * 16 + col

    loads = [
        pltpu.make_async_copy(far, near, load.at[k])
        for k, (far, near) in enumerate(
            (
                (x_far, x),
                (high_far, high),
                (low_far, low),
                (lanes_far, lanes),
                (place_far, place),
                (columns_far, columns),
                (inner_far, inner),
                (outer_far, outer),
            )
        )
    ]
    for one in loads:
        one.start()

    cols = [wrap(col + c, 16) for c in range(16)]

    def each_peer(act):
        def group(o, base):
            rows = [wrap(base + k, 8) for k in range(8)]
            for u in range(16):
                to_row, to_col = rows[(STEP * u // 16) % 8], cols[STEP * u % 16]
                if u == 0:
                    pl.when(o > 0)(functools.partial(act, to_row, to_col))
                else:
                    act(to_row, to_col)
            return wrap(base + STEP % 8, 8)

        lax.fori_loop(0, 8, group, row)

    at_x, at_core = lax.div(row, 2), lax.rem(row, 2)
    at_z, at_y = lax.div(col, 4), lax.rem(col, 4)
    to_x = [wrap(at_x + d, 4) * 2 for d in range(4)]
    to_core = [wrap(at_core + d, 2) for d in range(2)]
    to_z = [wrap(at_z + d, 4) * 4 for d in range(4)]
    to_y = [wrap(at_y + d, 4) for d in range(4)]

    def far_first(act):
        for dx, dc, dz, dy in FAR:
            act(to_x[dx] + to_core[dc], to_z[dz] + to_y[dy])

    barrier = pltpu.get_barrier_semaphore()

    def greet(to_row, to_col):
        pl.semaphore_signal(barrier, inc=1, device_id=(to_row, to_col), device_id_type=MESH)

    far_first(greet)
    loads[0].wait()
    pl.semaphore_wait(barrier, DEVICES - 1)

    def exchange(src_of, dst_of, phase, order=each_peer):
        mine = dst_of(me)

        def one(to_row, to_col):
            pltpu.make_async_remote_copy(
                src_ref=src_of(to_row * 16 + to_col),
                dst_ref=mine,
                send_sem=send.at[phase],
                recv_sem=recv.at[phase],
                device_id=(to_row, to_col),
                device_id_type=MESH,
            ).start()

        order(one)
        pltpu.make_async_copy(src_of(me), mine, recv.at[phase]).start()

    def arrived(ref, phase):
        pltpu.make_async_copy(ref, ref, recv.at[phase]).wait()

    def gone(ref, phase):
        pltpu.make_async_copy(ref, ref, send.at[phase]).wait()

    def first(h, carry):
        some = pl.ds(pl.multiple_of(8 * h, 8), 8)
        exchange(lambda q: x.at[:, q, some], lambda p: kept.at[h, pl.ds(2 * p, 2)], h)
        return carry

    lax.fori_loop(0, 2, first, 0)
    for one in loads[1:]:
        one.wait()

    here = lax.broadcasted_iota(jnp.int32, (128, 128), 1) == me

    def prepare(i, carry):
        own = [
            jnp.sum(jnp.where(here, place[i, r], 0.0), axis=1, keepdims=True) for r in range(2)
        ]
        base = lanes[i, 0], lanes[i, 1]
        for c in range(8):
            step = columns[i, :, c : c + 1], columns[i, :, 8 + c : 9 + c]
            re, im = times(times(own, step), base)
            turn1[i, c, 0], turn1[i, c, 1] = re, im
        for k in range(4):
            start[i, k] = jnp.broadcast_to(columns[i, :, 16 + k : 17 + k], (128, 128))
        return carry

    lax.fori_loop(0, 3, prepare, 0)
    for s in range(8):
        for r in range(2):
            turn2[s, r] = jnp.broadcast_to(columns[3, :, 8 * r + s : 8 * r + s + 1], (128, 128))
        re, im = times((inner[0], inner[1]), (outer[0, s : s + 1], outer[1, s : s + 1]))
        turn3[s, 0], turn3[s, 1] = re, im
    total[...] = jnp.zeros_like(total)

    kept_rows = kept.reshape(2, 2048, 128)
    sent_rows = sent.reshape(3, 2, 1024, 128)
    field_rows = field.reshape(3, 2, 1024, 128)
    back_rows = back.reshape(3, 2, 1024, 128)
    home_rows = home.reshape(3, 2, 1024, 128)
    final_rows = final.reshape(2, 2048, 128)

    def every(first_row):
        return pl.ds(first_row, 128, stride=8)

    def expand(j, carry):
        i = jnp.where(j < 4, lax.rem(j, 2), 2)
        h = jnp.where(j < 4, lax.div(j, 2), j - 4)

        @pl.when((j < 4) & (i == 0))
        def _():
            arrived(kept.at[h], h)

        by_low = start[i, 0], start[i, 1]
        by_high = start[i, 2], start[i, 3]
        for g in range(2):
            pair = []
            for c in (2 * g, 2 * g + 1):
                below = kept_rows[h, every(2 * c), :], kept_rows[h, every(2 * c + 1), :]
                above = (
                    kept_rows[h, every(1024 + 2 * c), :],
                    kept_rows[h, every(1025 + 2 * c), :],
                )
                pair.append(add(times(below, by_low), times(above, by_high)))
            mixed = from_left(high[0], low[0], paired(*pair))
            for w in range(2):
                c = 2 * g + w
                by = turn1[i, 4 * h + c, 0], turn1[i, 4 * h + c, 1]
                re, im = times(parts(mixed, w), by)
                sent_rows[i, h, every(c), :] = re
                sent_rows[i, h, every(4 + c), :] = im
        exchange(lambda q: sent.at[i, h, q], lambda p: field.at[i, h, p], 2 + 2 * i + h)
        return carry

    lax.fori_loop(0, 6, expand, 0)

    scale = 1.0 / math.sqrt(MODES)
    factor = 1.0 / math.sqrt(POINTS)

    def middle(i, carry):
        for h in range(2):
            arrived(field.at[i, h], 2 + 2 * i + h)
            for g in range(2):
                pair = [
                    (field_rows[i, h, every(s), :], field_rows[i, h, every(4 + s), :])
                    for s in (2 * g, 2 * g + 1)
                ]
                mixed = from_left(high[0], low[0], paired(*pair))
                for w in range(2):
                    s = 4 * h + 2 * g + w
                    work[s, 0], work[s, 1] = parts(mixed, w)

        def rise(k, inside):
            rows = pl.ds(pl.multiple_of(8 * k, 8), 8)
            v = [
                times(
                    (work[s, 0, rows, :], work[s, 1, rows, :]),
                    (turn2[s, 0, rows, :], turn2[s, 1, rows, :]),
                )
                for s in range(8)
            ]
            v = eight(v, 1)
            for s in range(8):
                re, im = times(v[s], (turn3[s, 0, rows, :], turn3[s, 1, rows, :]))
                work[s, 0, rows, :] = re
                work[s, 1, rows, :] = im
            return inside

        lax.fori_loop(0, 16, rise, 0)

        def peak(k, inside):
            some = pl.ds(4 * k, 4)
            value = jnp.concatenate(
                [work[some, 0].reshape(512, 128), work[some, 1].reshape(512, 128)], axis=1
            )
            value = from_right(value, high[1], low[1]) * scale
            re, im = value[:, :128], value[:, 128:]
            value = jnp.concatenate(
                [(re * re - im * im) * factor, (2.0 * factor) * (re * im)], axis=1
            )
            value = from_right(value, high[0], low[0])
            re, im = times_conj(
                (value[:, :128].reshape(4, 128, 128), value[:, 128:].reshape(4, 128, 128)),
                (turn3[some, 0], turn3[some, 1]),
            )
            work[some, 0] = re
            work[some, 1] = im
            return inside

        lax.fori_loop(0, 2, peak, 0)

        def fall(k, inside):
            rows = pl.ds(pl.multiple_of(8 * k, 8), 8)
            v = eight([(work[s, 0, rows, :], work[s, 1, rows, :]) for s in range(8)], -1)
            for s in range(8):
                re, im = times_conj(v[s], (turn2[s, 0, rows, :], turn2[s, 1, rows, :]))
                work[s, 0, rows, :] = re
                work[s, 1, rows, :] = im
            return inside

        lax.fori_loop(0, 16, fall, 0)

        def part(h, inside):
            for g in range(2):
                pair = [(work[4 * h + s, 0], work[4 * h + s, 1]) for s in (2 * g, 2 * g + 1)]
                mixed = from_left(high[1], low[1], paired(*pair))
                for w in range(2):
                    s = 2 * g + w
                    re, im = parts(mixed, w)
                    back_rows[i, h, every(s), :] = re
                    back_rows[i, h, every(4 + s), :] = im

            def give(k, within):
                exchange(
                    lambda q: back.at[k, h, q], lambda p: home.at[k, h, p], 8 + 2 * k + h
                )
                return within

            first_one = jnp.where(h == 0, i, 0)
            past_last = jnp.where(h == 0, i + 1, jnp.where(i == 2, 3, 0))
            lax.fori_loop(first_one, past_last, give, 0)
            return inside

        lax.fori_loop(0, 2, part, 0)
        return carry

    lax.fori_loop(0, 3, middle, 0)

    def gather(j, carry):
        i, h = lax.rem(j, 3), lax.div(j, 3)
        arrived(home.at[i, h], 8 + 2 * i + h)
        by_low = start[i, 0], start[i, 1]
        by_high = start[i, 2], start[i, 3]
        for g in range(2):
            pair = [
                times_conj(
                    (home_rows[i, h, every(c), :], home_rows[i, h, every(4 + c), :]),
                    (turn1[i, 4 * h + c, 0], turn1[i, 4 * h + c, 1]),
                )
                for c in (2 * g, 2 * g + 1)
            ]
            mixed = from_left(high[1], low[1], paired(*pair))
            for w in range(2):
                c = 2 * g + w
                value = parts(mixed, w)
                for f, by in enumerate((by_low, by_high)):
                    re, im = times_conj(value, by)
                    total[h, c, f, 0] += re
                    total[h, c, f, 1] += im

        @pl.when(i == 2)
        def _():
            for c in range(4):
                for f in range(2):
                    for r in range(2):
                        final_rows[h, every(1024 * f + 2 * c + r), :] = total[h, c, f, r]
            some = pl.ds(pl.multiple_of(8 * h, 8), 8)
            def give(order):
                exchange(
                    lambda q: final.at[h, pl.ds(2 * q, 2)],
                    lambda p: out.at[:, p, some],
                    14 + h,
                    order,
                )

            pl.when(h == 0)(functools.partial(give, each_peer))
            pl.when(h == 1)(functools.partial(give, far_first))

        return carry

    lax.fori_loop(0, 6, gather, 0)
    others = pl.ds(0, DEVICES - 1)
    double = pl.ds(0, 2 * (DEVICES - 1))
    for h in range(2):
        gone(kept.at[h, double], h)
        for i in range(3):
            gone(sent.at[i, h, others], 2 + 2 * i + h)
            gone(back.at[i, h, others], 8 + 2 * i + h)
    for h in range(2):
        arrived(final.at[h], 14 + h)
        gone(final.at[h, double], 14 + h)


def body(spectrum):
    x = spectrum.reshape(2, 2048, 128).transpose(1, 0, 2).reshape(2, 128, 16, 128)
    anywhere = pl.BlockSpec(memory_space=pl.ANY)
    held = [jnp.asarray(t) for t in tables()]
    grid = (3, 2, 128, 8, 128)
    out = pl.pallas_call(
        kernel,
        name="convolve",
        out_shape=pltpu.VMEM((2, 128, 16, 128), F32),
        in_specs=[anywhere] * (1 + len(held)),
        out_specs=anywhere,
        scratch_shapes=[
            pltpu.VMEM((2, 128, 16, 128), F32),
            *[pltpu.VMEM(t.shape, t.dtype) for t in held],
            pltpu.VMEM((2, 256, 8, 128), F32),
            pltpu.VMEM(grid, F32),
            pltpu.VMEM(grid, F32),
            pltpu.VMEM(grid, F32),
            pltpu.VMEM(grid, F32),
            pltpu.VMEM((2, 256, 8, 128), F32),
            pltpu.VMEM((2, 4, 2, 2, 128, 128), F32),
            pltpu.VMEM((8, 2, 128, 128), F32),
            pltpu.VMEM((3, 8, 2, 128, 128), F32),
            pltpu.VMEM((8, 2, 128, 128), F32),
            pltpu.VMEM((8, 2, 128, 128), F32),
            pltpu.VMEM((3, 4, 128, 128), F32),
            pltpu.SemaphoreType.DMA((8,)),
            pltpu.SemaphoreType.DMA((16,)),
            pltpu.SemaphoreType.DMA((16,)),
        ],
        compiler_params=pltpu.CompilerParams(
            collective_id=0, has_side_effects=True, vmem_limit_bytes=40 * 1024 * 1024
        ),
    )(*[pltpu.with_memory_space_constraint(t, pltpu.HBM) for t in (x, *held)])
    return out.reshape(2048, 2, 128).transpose(1, 0, 2).reshape(2, 262144)


def solution(mesh):
    return jax.shard_map(
        body,
        mesh=mesh,
        in_specs=(P(None, ("row", "col")),),
        out_specs=P(None, ("row", "col")),
        check_vma=False,
    )
```
